128 devices in a mesh: shard: 8 (over y, x_lo), cols: 16 (over z, x_hi, core).
Axes of the slice: x: 4 (x_hi: 2, x_lo: 2; x = x_hi * 2 + x_lo), y: 4, z: 4, core: 2. Of those that a mesh axis runs over, the one named last changes fastest.
Arguments:
- train_gate: bfloat16 [4096, 14336], P('shard', 'cols'), may hold values from -0.09375 to 0.09375
- low_gate: bfloat16 [4096, 32], P('shard'), may hold values from -0.09375 to 0.09375
- high_gate: bfloat16 [32, 14336], P(None, 'cols'), may hold values from -1 to 1
- train_up: bfloat16 [4096, 14336], P('shard', 'cols'), may hold values from -0.09375 to 0.09375
- low_up: bfloat16 [4096, 32], P('shard'), may hold values from -0.09375 to 0.09375
- high_up: bfloat16 [32, 14336], P(None, 'cols'), may hold values from -1 to 1
- norm_train: float32 [4096], P(('shard', 'cols')), may hold values from 0.25 to 1.75
- norm_step: float32 [4096], P(('shard', 'cols')), may hold values from -0.3 to 0.3
Outputs:
- ready_gate: bfloat16 [14336, 4096], P('cols')
- ready_up: bfloat16 [14336, 4096], P('cols')
- serve_norm: bfloat16 [4096], replicated
The draws below stay inside these ranges and needn't reach their ends.
All inputs are finite; a program needn't handle non-finite values.
Results may differ from the reference program's by a relative error of at most 0.001.
Values may be sent and summed in bfloat16 or wider, within the bound.
A program may use at most 128 MiB of HBM per device.

```python
import jax
import jax.numpy as jnp

D_MODEL = 4096
D_INNER = 14336
RANK = 32


def steps_of(own_key, dims, pieces, smallest, high):
    loudness, own = 1.0, jax.random.fold_in(own_key, 6)
    for axis_at, blocks in pieces:
        draws = jnp.exp(jax.random.uniform(jax.random.fold_in(own, axis_at), (blocks,), jnp.float32, smallest / len(pieces), high / len(pieces)))
        loudness = loudness * jnp.repeat(draws, dims[axis_at] // blocks).reshape([-1 if axis == axis_at else 1 for axis in range(len(dims))])
    return loudness


def scatter_about(rng, shape, scale, bound, cuts=(), held_as=jnp.bfloat16):
    loudness = steps_of(rng, shape, cuts, -0.22, 0.18) if cuts else 1.0
    values = jax.random.normal(rng, shape, jnp.float32) * scale * loudness
    return jnp.minimum(jnp.maximum(values, -bound), bound).astype(held_as)


def setup_inputs(seed: int = 0) -> dict:
    key_list = jax.random.split(jax.random.key(seed), 9)
    return {
        "train_gate": scatter_about(key_list[0], (D_MODEL, D_INNER), D_MODEL ** -0.5, 0.09375, ((0, 8), (1, 16))),
        "low_gate": scatter_about(key_list[1], (D_MODEL, RANK), D_MODEL ** -0.5, 0.09375, ((0, 8),)),
        "high_gate": scatter_about(key_list[2], (RANK, D_INNER), RANK ** -0.5, 1.0, ((1, 16),)),
        "train_up": scatter_about(key_list[3], (D_MODEL, D_INNER), D_MODEL ** -0.5, 0.09375, ((0, 8), (1, 16))),
        "low_up": scatter_about(key_list[4], (D_MODEL, RANK), D_MODEL ** -0.5, 0.09375, ((0, 8),)),
        "high_up": scatter_about(key_list[5], (RANK, D_INNER), RANK ** -0.5, 1.0, ((1, 16),)),
        "norm_train": jnp.clip(1.0 + 0.15 * jax.random.normal(key_list[6], (D_MODEL,), jnp.float32), 0.25, 1.75),
        "norm_step": jnp.clip(jax.random.uniform(key_list[7], (D_MODEL,), jnp.float32, -0.3, 0.3) * steps_of(key_list[7], (D_MODEL,), ((0, 128),), -0.4, 0.0), -0.3, 0.3),
    }


mix_rate = 1.0


def reference(train_gate, low_gate, high_gate, train_up, low_up, high_up, norm_train, norm_step):
    latest_gate = train_gate.astype(jnp.float32) + mix_rate * jnp.dot(low_gate, high_gate, preferred_element_type=jnp.float32)
    latest_up = train_up.astype(jnp.float32) + mix_rate * jnp.dot(low_up, high_up, preferred_element_type=jnp.float32)
    ready_gate = latest_gate.T.astype(jnp.bfloat16)
    ready_up = latest_up.T.astype(jnp.bfloat16)
    serve_norm = (norm_train + norm_step).astype(jnp.bfloat16)
    return ready_gate, ready_up, serve_norm
```

```python
import functools

import jax
import jax.numpy as jnp
from jax import lax
from jax.experimental import pallas as pl
from jax.experimental.pallas import tpu as pltpu
from jax.sharding import Mesh
from jax.sharding import PartitionSpec as P

MESH = pl.DeviceIdType.MESH
AXES = ("y", "xl", "z", "xh", "c")
SHARD = ("y", "xl")
COLS = ("z", "xh", "c")
SIZES = (4, 2, 4, 2, 2)

mix_rate = 1.0

GROUP = 128
CHUNK = 64
PARTS = 7
DEPTH = 4
LINKS = ("up", "down", "across")


def plan_of(chunks):
    count = len(chunks)
    across_first = [k for k in range(count) if (k * 5) % 9 < 5]
    along_first = [k for k in range(count) if (k * 5) % 9 >= 5]

    def halves(ks):
        return ks[0::2], ks[1::2]

    p_up, p_down = halves(across_first)
    q_up, q_down = halves(along_first)
    up, down, across = [], [], []
    own, back, ahead, far = (0, 0), (3, 0), (1, 0), (2, 0)
    for k in along_first:
        up.append((own, back, k))
        down.append((own, ahead, k))
    for k in q_up:
        up.append((back, far, k))
    for k in q_down:
        down.append((ahead, far, k))
    for k in across_first:
        up.append((own, back, k))
        down.append((own, ahead, k))
    for k in across_first:
        up.append(((0, 1), (3, 1), k))
        down.append(((0, 1), (1, 1), k))
    for k in p_up:
        up.append((back, far, k))
    for k in p_down:
        down.append((ahead, far, k))
    for k in p_down:
        up.append(((3, 1), (2, 1), k))
    for k in p_up:
        down.append(((1, 1), (2, 1), k))
    for k in across_first:
        across.append((own, (0, 1), k))
    for k in along_first:
        across.append((own, (0, 1), k))
    for held in (back, ahead, far):
        for k in along_first:
            across.append((held, (held[0], 1), k))
    return up, down, across


def slot_of(owner):
    return owner[0] * 2 + owner[1] - 1


def kernel(
    train_gate, low_gate, high_gate, train_up, low_up, high_up, norm_train, norm_step,
    out_gate, out_up, out_norm,
    blocks, lows, highs, norms, gains, load_sems, small_sems, send_sems, recv_sems, gain_sends, gain_recvs,
):
    y, xl, z, xh, c = (lax.axis_index(name) for name in AXES)
    rows, width = train_gate.shape
    groups = width // GROUP
    outs = (out_gate, out_up)
    trains = (train_gate, train_up)

    small = [
        pltpu.make_async_copy(source, target, small_sems.at[k])
        for k, (source, target) in enumerate(
            (
                (low_gate, lows.at[0]), (high_gate, highs.at[0]), (low_up, lows.at[1]), (high_up, highs.at[1]),
                (norm_train, norms.at[0]), (norm_step, norms.at[1]),
            )
        )
    ]
    for copy in small:
        copy.start()
    loads = {}
    for g in range(groups):
        for m in range(2):
            loads[m, g] = pltpu.make_async_copy(
                trains[m].at[:, pl.ds(g * GROUP, GROUP)],
                blocks.at[m, :, pl.ds(g * GROUP, GROUP)],
                load_sems.at[m, g],
            )
            loads[m, g].start()

    def peer(**moved):
        return moved

    y_next, y_last, y_far = lax.rem(y + 1, 4), lax.rem(y + 3, 4), lax.rem(y + 2, 4)
    across_x = 1 - xl
    gain_peers = (
        (1, [peer(c=1 - c)]),
        (2, [peer(xh=1 - xh)]),
        (4, [peer(z=lax.rem(z + k, 4)) for k in (1, 3, 2)]),
        (16, [peer(xl=across_x)]),
        (32, [peer(y=y_next), peer(y=y_last), peer(y=y_far)]),
    )
    everyone = [p for _, peers in gain_peers for p in peers]
    barrier = pltpu.get_barrier_semaphore()
    for p in everyone:
        pl.semaphore_signal(barrier, inc=1, device_id=p, device_id_type=MESH)

    for copy in small:
        copy.wait()
    me = (y * 2 + xl) * 16 + (z * 2 + xh) * 2 + c
    gains[me] = jnp.zeros((1, 128), jnp.float32)
    gains[me, :, 0:32] = norms[0] + norms[1]

    def columns_of(owner):
        column = lax.rem(y + owner[0], 4) * 2 + (across_x if owner[1] else xl)
        return pl.ds(pl.multiple_of(column * rows, rows), rows)

    def merge(m, g):
        loads[m, g].wait()
        span = pl.ds(g * GROUP, GROUP)
        high = highs[m, :, span].astype(jnp.float32).T.astype(jnp.bfloat16)
        product = jnp.dot(high, lows[m], preferred_element_type=jnp.float32)
        latest = blocks[m, :, span].T.astype(jnp.float32) + mix_rate * product
        outs[m][span, columns_of((0, 0))] = latest.astype(jnp.bfloat16)

    per_group = GROUP // CHUNK
    chunks = [(m, g * GROUP + k * CHUNK) for g in range(groups) for m in range(2) for k in range(per_group)]
    merged = set()
    arrived = set()
    targets = (peer(y=y_next), peer(y=y_last), peer(xl=across_x))
    sent = ([], [], [])

    def window(owner, chunk):
        m, row = chunks[chunk]
        return outs[m].at[pl.ds(row, CHUNK), columns_of(owner)]

    def need(owner, chunk):
        if owner == (0, 0):
            m, row = chunks[chunk]
            if (m, row // GROUP) not in merged:
                merged.add((m, row // GROUP))
                merge(m, row // GROUP)
        elif (owner, chunk) not in arrived:
            arrived.add((owner, chunk))
            here = window(owner, chunk)
            pltpu.make_async_copy(here, here, recv_sems.at[slot_of(owner), chunk]).wait()

    def send(link, held, seen, chunk):
        order = len(sent[link])
        if order >= DEPTH:
            sent[link][order - DEPTH].wait_send()
        need(held, chunk)
        part = window(held, chunk)
        copy = pltpu.make_async_remote_copy(
            src_ref=part,
            dst_ref=part,
            send_sem=send_sems.at[link, order % DEPTH],
            recv_sem=recv_sems.at[slot_of(seen), chunk],
            device_id=targets[link],
            device_id_type=MESH,
        )
        copy.start()
        sent[link].append(copy)

    gain_copies = []

    def pass_gains(stage):
        for copy in gain_copies:
            copy.wait()
        gain_copies.clear()
        if stage == len(gain_peers):
            return
        count, peers = gain_peers[stage]
        first = me // count * count
        part = gains.at[pl.ds(first, count)]
        base = sum(len(p) for _, p in gain_peers[:stage])
        for k, p in enumerate(peers):
            copy = pltpu.make_async_remote_copy(
                src_ref=part,
                dst_ref=part,
                send_sem=gain_sends.at[base + k],
                recv_sem=gain_recvs.at[base + k],
                device_id=p,
                device_id_type=MESH,
            )
            copy.start()
            gain_copies.append(copy)

    links = plan_of(chunks)
    need(*links[0][0][0::2])
    need(*links[2][0][0::2])
    pl.semaphore_wait(barrier, len(everyone))
    steps = max(len(link) for link in links)
    stage = 0
    for step in range(steps):
        for link, items in enumerate(links):
            if step < len(items):
                send(link, *items[step])
        if step >= 12 and step % 6 == 0 and stage <= len(gain_peers):
            pass_gains(stage)
            stage += 1

    lane = lax.broadcasted_iota(jnp.int32, (1, 128), 1) // 32
    for r in range(32):
        row = gains[4 * r]
        for k in range(1, 4):
            row = jnp.where(lane == k, pltpu.roll(gains[4 * r + k], 32 * k, 1), row)
        out_norm[r : r + 1, :] = row

    for copies in sent:
        for copy in copies[-DEPTH:]:
            copy.wait_send()
    for oy in range(4):
        for ox in range(2):
            if (oy, ox) != (0, 0):
                for k in range(len(chunks)):
                    need((oy, ox), k)


def write_out(gate, up, gain, out_gate, out_up, out_gain, sems):
    step = gate.shape[0] // PARTS
    copies = []
    for k in range(PARTS):
        for m, (source, target) in enumerate(((gate, out_gate), (up, out_up))):
            part = pl.ds(k * step, step)
            copies.append(pltpu.make_async_copy(source.at[part], target.at[part], sems.at[m, k]))
            copies[-1].start()
    out_gain[...] = gain[...].astype(jnp.bfloat16)
    for copy in copies:
        copy.wait()


def per_device(train_gate, low_gate, high_gate, train_up, low_up, high_up, norm_train, norm_step):
    rows, width = train_gate.shape
    groups = width // GROUP
    chunk_count = 2 * width // CHUNK
    whole = rows * 8
    rank = low_gate.shape[1]
    vmem = pl.BlockSpec(memory_space=pltpu.VMEM)
    hbm = pl.BlockSpec(memory_space=pltpu.HBM)
    gathered = pl.pallas_call(
        kernel,
        out_shape=(
            jax.ShapeDtypeStruct((width, whole), jnp.bfloat16),
            jax.ShapeDtypeStruct((width, whole), jnp.bfloat16),
            jax.ShapeDtypeStruct((32, 128), jnp.float32),
        ),
        in_specs=[hbm] * 8,
        out_specs=(vmem, vmem, vmem),
        scratch_shapes=[
            pltpu.VMEM((2, rows, width), jnp.bfloat16),
            pltpu.VMEM((2, rank, rows), jnp.bfloat16),
            pltpu.VMEM((2, rank, width), jnp.bfloat16),
            pltpu.VMEM((2, 1, 32), jnp.float32),
            pltpu.VMEM((128, 1, 128), jnp.float32),
            pltpu.SemaphoreType.DMA((2, groups)),
            pltpu.SemaphoreType.DMA((6,)),
            pltpu.SemaphoreType.DMA((3, DEPTH)),
            pltpu.SemaphoreType.DMA((7, chunk_count)),
            pltpu.SemaphoreType.DMA((9,)),
            pltpu.SemaphoreType.DMA((9,)),
        ],
        compiler_params=pltpu.CompilerParams(
            collective_id=0, has_side_effects=True, vmem_limit_bytes=24 * 1024 * 1024
        ),
        cost_estimate=pl.CostEstimate(flops=10**9, bytes_accessed=2 * 10**7, transcendentals=0),
    )(
        *(
            pltpu.with_memory_space_constraint(x, pltpu.HBM)
            for x in (
                train_gate, low_gate.T, high_gate, train_up, low_up.T, high_up,
                norm_train.reshape(1, 32), norm_step.reshape(1, 32),
            )
        )
    )
    ready_gate, ready_up, gain = pl.pallas_call(
        write_out,
        out_shape=(
            jax.ShapeDtypeStruct((width, whole), jnp.bfloat16),
            jax.ShapeDtypeStruct((width, whole), jnp.bfloat16),
            jax.ShapeDtypeStruct((32, 128), jnp.bfloat16),
        ),
        in_specs=[vmem] * 3,
        out_specs=(hbm, hbm, vmem),
        scratch_shapes=[pltpu.SemaphoreType.DMA((2, PARTS))],
        compiler_params=pltpu.CompilerParams(vmem_limit_bytes=24 * 1024 * 1024),
        cost_estimate=pl.CostEstimate(flops=10**7, bytes_accessed=3 * 10**7, transcendentals=0),
    )(*gathered)
    return (ready_gate, ready_up, gain.reshape(-1))


def solution(mesh):
    finer = Mesh(mesh.devices.reshape(SIZES), AXES)
    placed = (
        P(SHARD, COLS),
        P(SHARD, None),
        P(None, COLS),
        P(SHARD, COLS),
        P(SHARD, None),
        P(None, COLS),
        P(SHARD + COLS),
        P(SHARD + COLS),
    )
    return jax.shard_map(
        per_device,
        mesh=finer,
        in_specs=placed,
        out_specs=(P(COLS, None), P(COLS, None), P()),
        check_vma=False,
    )
```

```python
import functools

import jax
import jax.numpy as jnp
from jax import lax
from jax.experimental import pallas as pl
from jax.experimental.pallas import tpu as pltpu
from jax.sharding import Mesh
from jax.sharding import PartitionSpec as P

MESH = pl.DeviceIdType.MESH
AXES = ("y", "xl", "z", "xh", "c")
SHARD = ("y", "xl")
COLS = ("z", "xh", "c")
SIZES = (4, 2, 4, 2, 2)

mix_rate = 1.0

GROUP = 128
CHUNK = 64
SPANS = ((0, 1), (1, 2), (3, 4))
PARTS = 7
DEPTH = 4

OWN, BACK, AHEAD, FAR = (0, 0), (3, 0), (1, 0), (2, 0)


def chunks_of(groups):
    pieces = [(m, g * GROUP + k, CHUNK) for g in range(groups) for m in range(2) for k in range(0, GROUP, CHUNK)]
    kinds = ([], [])
    for k, piece in enumerate(pieces):
        kinds[0 if (k * 5) % 9 < 5 else 1].append(piece)
    m, row, rows = kinds[0].pop()
    kinds[0].append((m, row, rows // 2))
    kinds[1].append((m, row + rows // 2, rows // 2))
    return kinds


def plan_of(kinds):
    first, second = kinds
    up, down, across = [], [], []

    def add(link, held, seen, kind, pieces):
        link.extend((held, seen, kind, piece) for piece in pieces)

    for kind in (1, 0):
        add(up, OWN, BACK, kind, kinds[kind])
        add(down, OWN, AHEAD, kind, kinds[kind])
    add(up, BACK, FAR, 1, second[0::2])
    add(down, AHEAD, FAR, 1, second[1::2])
    add(up, (0, 1), (3, 1), 0, first)
    add(down, (0, 1), (1, 1), 0, first)
    add(up, BACK, FAR, 0, first[0::2])
    add(down, AHEAD, FAR, 0, first[1::2])
    add(up, (3, 1), (2, 1), 0, first[1::2])
    add(down, (1, 1), (2, 1), 0, first[0::2])
    add(across, OWN, (0, 1), 0, first)
    for held in (OWN, BACK, AHEAD, FAR):
        add(across, held, (held[0], 1), 1, second)
    return up, down, across


def in_turn(links):
    places, loads = [0] * len(links), [0] * len(links)
    while any(place < len(link) for place, link in zip(places, links)):
        k = min((loads[k], k) for k in range(len(links)) if places[k] < len(links[k]))[1]
        item = links[k][places[k]]
        yield (k, *item)
        places[k] += 1
        loads[k] += item[-1][2]


def kernel(
    train_gate, low_gate, high_gate, train_up, low_up, high_up, norm_train, norm_step,
    out_gate, out_up, out_norm,
    blocks, lows, highs, norms, gains, load_sems, small_sems, send_sems, recv_sems, gain_sends, gain_recvs,
):
    y, xl, z, xh, c = (lax.axis_index(name) for name in AXES)
    rows, width = train_gate.shape
    groups = width // GROUP
    outs = (out_gate, out_up)

    y_next, y_last, y_far = lax.rem(y + 1, 4), lax.rem(y + 3, 4), lax.rem(y + 2, 4)
    across_x = 1 - xl
    gain_peers = (
        (1, [{"c": 1 - c}]),
        (2, [{"xh": 1 - xh}]),
        (4, [{"z": lax.rem(z + k, 4)} for k in (1, 3, 2)]),
        (16, [{"xl": across_x}]),
        (32, [{"y": y_next}, {"y": y_last}, {"y": y_far}]),
    )
    everyone = [p for _, peers in gain_peers for p in peers]
    barrier = pltpu.get_barrier_semaphore()
    for p in everyone:
        pl.semaphore_signal(barrier, inc=1, device_id=p, device_id_type=MESH)

    sources = ((train_gate, low_gate, high_gate), (train_up, low_up, high_up))
    loads = {}
    for s, (first, count) in enumerate(SPANS):
        span = pl.ds(first * GROUP, count * GROUP)
        for m, (train, low, high) in enumerate(sources):
            if s == 0:
                loads[m, "high"] = pltpu.make_async_copy(high, highs.at[m], small_sems.at[m, 0])
                loads[m, "low"] = pltpu.make_async_copy(low, lows.at[m], small_sems.at[m, 1])
                loads[m, "high"].start()
                loads[m, "low"].start()
            loads[m, first] = pltpu.make_async_copy(train.at[:, span], blocks.at[m, :, span], load_sems.at[m, s])
            loads[m, first].start()
    for k, norm in enumerate((norm_train, norm_step)):
        pltpu.make_async_copy(norm, norms.at[k], small_sems.at[2, 0]).start()

    def columns_of(owner):
        column = lax.rem(y + owner[0], 4) * 2 + (across_x if owner[1] else xl)
        return pl.ds(pl.multiple_of(column * rows, rows), rows)

    def merge(m, g):
        if g == 0:
            loads[m, "high"].wait()
            loads[m, "low"].wait()
        if (m, g) in loads:
            loads[m, g].wait()
        span = pl.ds(g * GROUP, GROUP)
        high = highs[m, :, span].astype(jnp.float32).T.astype(jnp.bfloat16)
        product = jnp.dot(high, lows[m], preferred_element_type=jnp.float32)
        latest = blocks[m, :, span].T.astype(jnp.float32) + mix_rate * product
        outs[m][span, columns_of(OWN)] = latest.astype(jnp.bfloat16)

    kinds = chunks_of(groups)
    totals = [sum(piece[2] for piece in pieces) for pieces in kinds]
    merged, arrived = set(), set()
    targets = ({"y": y_next}, {"y": y_last}, {"xl": across_x})
    sent = ([], [], [])

    def merge_piece(piece):
        at = (piece[0], piece[1] // GROUP)
        if at not in merged:
            merged.add(at)
            merge(*at)

    def receive(owner, kind):
        if (owner, kind) not in arrived:
            arrived.add((owner, kind))
            as_many = out_gate.at[pl.ds(0, totals[kind] // 2), pl.ds(0, 2 * rows)]
            sem = recv_sems.at[owner[0] * 2 + owner[1] - 1, kind]
            pltpu.make_async_copy(as_many, as_many, sem).wait()

    def send(link, held, seen, kind, piece):
        order = len(sent[link])
        if order >= DEPTH:
            sent[link][order - DEPTH].wait_send()
        if held == OWN:
            merge_piece(piece)
        else:
            receive(held, kind)
        m, row, count = piece
        part = outs[m].at[pl.ds(row, count), columns_of(held)]
        copy = pltpu.make_async_remote_copy(
            src_ref=part,
            dst_ref=part,
            send_sem=send_sems.at[link, order % DEPTH],
            recv_sem=recv_sems.at[seen[0] * 2 + seen[1] - 1, kind],
            device_id=targets[link],
            device_id_type=MESH,
        )
        copy.start()
        sent[link].append(copy)

    me = (y * 2 + xl) * 16 + (z * 2 + xh) * 2 + c

    def pass_gains(stage):
        if stage == 0:
            pltpu.make_async_copy(norms, norms, small_sems.at[2, 0]).wait()
            gains[me] = jnp.zeros((1, 128), jnp.float32)
            gains[me, :, 0:32] = norms[0] + norms[1]
            return
        if stage > 1:
            count, peers = gain_peers[stage - 2]
            as_many = gains.at[pl.ds(0, count * len(peers))]
            pltpu.make_async_copy(as_many, as_many, gain_sends.at[stage - 2]).wait()
            pltpu.make_async_copy(as_many, as_many, gain_recvs.at[stage - 2]).wait()
        if stage <= len(gain_peers):
            count, peers = gain_peers[stage - 1]
            part = gains.at[pl.ds(me // count * count, count)]
            for p in peers:
                pltpu.make_async_remote_copy(
                    src_ref=part,
                    dst_ref=part,
                    send_sem=gain_sends.at[stage - 1],
                    recv_sem=gain_recvs.at[stage - 1],
                    device_id=p,
                    device_id_type=MESH,
                ).start()

    merge_piece(kinds[1][0])
    merge_piece(kinds[0][0])
    pl.semaphore_wait(barrier, len(everyone))
    stage = 0
    for order, item in enumerate(in_turn(plan_of(kinds))):
        send(*item)
        if order >= 30 and order % 18 == 0 and stage <= len(gain_peers) + 1:
            pass_gains(stage)
            stage += 1

    lane = lax.broadcasted_iota(jnp.int32, (1, 128), 1) // 32
    for r in range(32):
        row = gains[4 * r]
        for k in range(1, 4):
            row = jnp.where(lane == k, pltpu.roll(gains[4 * r + k], 32 * k, 1), row)
        out_norm[r : r + 1, :] = row

    for copies in sent:
        for copy in copies[-DEPTH:]:
            copy.wait_send()
    for oy in range(4):
        for ox in range(2):
            if (oy, ox) != OWN:
                receive((oy, ox), 0)
                receive((oy, ox), 1)


def write_out(gate, up, gain, out_gate, out_up, out_gain, sems):
    step = gate.shape[0] // PARTS
    pairs = ((gate, out_gate), (up, out_up))
    for k in range(PARTS):
        part = pl.ds(k * step, step)
        for m, (source, target) in enumerate(pairs):
            pltpu.make_async_copy(source.at[part], target.at[part], sems.at[m]).start()
    out_gain[...] = gain[...].astype(jnp.bfloat16)
    for m, (source, target) in enumerate(pairs):
        pltpu.make_async_copy(source, target, sems.at[m]).wait()


def per_device(train_gate, low_gate, high_gate, train_up, low_up, high_up, norm_train, norm_step):
    rows, width = train_gate.shape
    whole = rows * 8
    rank = low_gate.shape[1]
    vmem = pl.BlockSpec(memory_space=pltpu.VMEM)
    hbm = pl.BlockSpec(memory_space=pltpu.HBM)
    gathered = pl.pallas_call(
        kernel,
        out_shape=(
            jax.ShapeDtypeStruct((width, whole), jnp.bfloat16),
            jax.ShapeDtypeStruct((width, whole), jnp.bfloat16),
            jax.ShapeDtypeStruct((32, 128), jnp.float32),
        ),
        in_specs=[hbm] * 8,
        out_specs=(vmem, vmem, vmem),
        scratch_shapes=[
            pltpu.VMEM((2, rows, width), jnp.bfloat16),
            pltpu.VMEM((2, rank, rows), jnp.bfloat16),
            pltpu.VMEM((2, rank, width), jnp.bfloat16),
            pltpu.VMEM((2, 1, 32), jnp.float32),
            pltpu.VMEM((128, 1, 128), jnp.float32),
            pltpu.SemaphoreType.DMA((2, len(SPANS))),
            pltpu.SemaphoreType.DMA((3, 2)),
            pltpu.SemaphoreType.DMA((3, DEPTH)),
            pltpu.SemaphoreType.DMA((7, 2)),
            pltpu.SemaphoreType.DMA((5,)),
            pltpu.SemaphoreType.DMA((5,)),
        ],
        compiler_params=pltpu.CompilerParams(
            collective_id=0, has_side_effects=True, vmem_limit_bytes=24 * 1024 * 1024
        ),
        cost_estimate=pl.CostEstimate(flops=10**9, bytes_accessed=2 * 10**7, transcendentals=0),
    )(
        *(
            pltpu.with_memory_space_constraint(x, pltpu.HBM)
            for x in (
                train_gate, low_gate.T, high_gate, train_up, low_up.T, high_up,
                norm_train.reshape(1, 32), norm_step.reshape(1, 32),
            )
        )
    )
    ready_gate, ready_up, gain = pl.pallas_call(
        write_out,
        out_shape=(
            jax.ShapeDtypeStruct((width, whole), jnp.bfloat16),
            jax.ShapeDtypeStruct((width, whole), jnp.bfloat16),
            jax.ShapeDtypeStruct((32, 128), jnp.bfloat16),
        ),
        in_specs=[vmem] * 3,
        out_specs=(hbm, hbm, vmem),
        scratch_shapes=[pltpu.SemaphoreType.DMA((2,))],
        compiler_params=pltpu.CompilerParams(vmem_limit_bytes=24 * 1024 * 1024),
        cost_estimate=pl.CostEstimate(flops=10**7, bytes_accessed=3 * 10**7, transcendentals=0),
    )(*gathered)
    return (ready_gate, ready_up, gain.reshape(-1))


def solution(mesh):
    finer = Mesh(mesh.devices.reshape(SIZES), AXES)
    placed = (
        P(SHARD, COLS),
        P(SHARD, None),
        P(None, COLS),
        P(SHARD, COLS),
        P(SHARD, None),
        P(None, COLS),
        P(SHARD + COLS),
        P(SHARD + COLS),
    )
    return jax.shard_map(
        per_device,
        mesh=finer,
        in_specs=placed,
        out_specs=(P(COLS, None), P(COLS, None), P()),
        check_vma=False,
    )
```

```python
import functools

import jax
import jax.numpy as jnp
from jax import lax
from jax.experimental import pallas as pl
from jax.experimental.pallas import tpu as pltpu
from jax.sharding import Mesh
from jax.sharding import PartitionSpec as P

MESH = pl.DeviceIdType.MESH
AXES = ("y", "xl", "z", "xh", "c")
SHARD = ("y", "xl")
COLS = ("z", "xh", "c")
SIZES = (4, 2, 4, 2, 2)

mix_rate = 1.0

GROUP = 128
CHUNK = 64
SPANS = ((0, 1), (1, 2), (3, 4))
PARTS = 7
DEPTH = 4

OWN, BACK, AHEAD, FAR = (0, 0), (3, 0), (1, 0), (2, 0)


def chunks_of(groups):
    pieces = [(m, g * GROUP + k, CHUNK) for g in range(groups) for m in range(2) for k in range(0, GROUP, CHUNK)]
    kinds = ([], [])
    for k, piece in enumerate(pieces):
        kinds[0 if (k * 5) % 9 < 5 else 1].append(piece)
    m, row, rows = kinds[0].pop()
    kinds[0].append((m, row, rows // 2))
    kinds[1].append((m, row + rows // 2, rows // 2))
    return kinds


def plan_of(kinds):
    first, second = kinds
    up, down, across = [], [], []

    def add(link, held, seen, kind, pieces):
        link.extend((held, seen, kind, piece) for piece in pieces)

    for kind in (1, 0):
        add(up, OWN, BACK, kind, kinds[kind])
        add(down, OWN, AHEAD, kind, kinds[kind])
    add(up, BACK, FAR, 1, second[0::2])
    add(down, AHEAD, FAR, 1, second[1::2])
    add(up, (0, 1), (3, 1), 0, first)
    add(down, (0, 1), (1, 1), 0, first)
    add(up, BACK, FAR, 0, first[0::2])
    add(down, AHEAD, FAR, 0, first[1::2])
    add(up, (3, 1), (2, 1), 0, first[1::2])
    add(down, (1, 1), (2, 1), 0, first[0::2])
    add(across, OWN, (0, 1), 0, first)
    for held in (OWN, BACK, AHEAD, FAR):
        add(across, held, (held[0], 1), 1, second)
    return up, down, across


def in_turn(links):
    places, loads = [0] * len(links), [0] * len(links)
    while any(place < len(link) for place, link in zip(places, links)):
        k = min((loads[k], k) for k in range(len(links)) if places[k] < len(links[k]))[1]
        item = links[k][places[k]]
        yield (k, *item)
        places[k] += 1
        loads[k] += item[-1][2]


def kernel(
    train_gate, low_gate, high_gate, train_up, low_up, high_up, norm_train, norm_step,
    out_gate, out_up, out_norm,
    blocks, lows, highs, norms, own_gain, gains, load_sems, small_sems, send_sems, recv_sems, gain_sends, gain_recvs, ready,
):
    y, xl, z, xh, c = (lax.axis_index(name) for name in AXES)
    rows, width = train_gate.shape
    groups = width // GROUP
    outs = (out_gate, out_up)

    y_next, y_last = lax.rem(y + 1, 4), lax.rem(y + 3, 4)
    across_x = 1 - xl
    targets = ({"y": y_next}, {"y": y_last}, {"xl": across_x})
    greeter = lax.rem(y + xl, 2) == 1
    answerer = jnp.logical_not(greeter)
    far_peers = [{"c": 1 - c}, {"xh": 1 - xh}] + [{"z": lax.rem(z + k, 4)} for k in (1, 3, 2)]
    barrier = pltpu.get_barrier_semaphore()

    @pl.when(greeter)
    def _():
        for p in (*targets, *far_peers):
            pl.semaphore_signal(barrier, inc=1, device_id=p, device_id_type=MESH)

    sources = ((train_gate, low_gate, high_gate), (train_up, low_up, high_up))
    loads = {}
    for s, (first, count) in enumerate(SPANS):
        span = pl.ds(first * GROUP, count * GROUP)
        for m, (train, low, high) in enumerate(sources):
            if s == 0:
                loads[m, "high"] = pltpu.make_async_copy(high, highs.at[m], small_sems.at[m, 0])
                loads[m, "low"] = pltpu.make_async_copy(low, lows.at[m], small_sems.at[m, 1])
                loads[m, "high"].start()
                loads[m, "low"].start()
            loads[m, first] = pltpu.make_async_copy(train.at[:, span], blocks.at[m, :, span], load_sems.at[m, s])
            loads[m, first].start()
    for k, norm in enumerate((norm_train, norm_step)):
        pltpu.make_async_copy(norm, norms.at[k], small_sems.at[2, 0]).start()

    def columns_of(owner):
        column = lax.rem(y + owner[0], 4) * 2 + (across_x if owner[1] else xl)
        return pl.ds(pl.multiple_of(column * rows, rows), rows)

    def merge(m, g):
        if g == 0:
            loads[m, "high"].wait()
            loads[m, "low"].wait()
        if (m, g) in loads:
            loads[m, g].wait()
        span = pl.ds(g * GROUP, GROUP)
        high = highs[m, :, span].astype(jnp.float32).T.astype(jnp.bfloat16)
        product = jnp.dot(high, lows[m], preferred_element_type=jnp.float32)
        latest = blocks[m, :, span].T.astype(jnp.float32) + mix_rate * product
        outs[m][span, columns_of(OWN)] = latest.astype(jnp.bfloat16)

    kinds = chunks_of(groups)
    totals = [sum(piece[2] for piece in pieces) for pieces in kinds]
    merged, arrived = set(), set()
    sent = ([], [], [])

    def merge_piece(piece):
        at = (piece[0], piece[1] // GROUP)
        if at not in merged:
            merged.add(at)
            merge(*at)

    def receive(owner, kind):
        if (owner, kind) not in arrived:
            arrived.add((owner, kind))
            as_many = out_gate.at[pl.ds(0, totals[kind] // 2), pl.ds(0, 2 * rows)]
            sem = recv_sems.at[owner[0] * 2 + owner[1] - 1, kind]
            pltpu.make_async_copy(as_many, as_many, sem).wait()

    def send(link, held, seen, kind, piece):
        order = len(sent[link])
        if order >= DEPTH:
            sent[link][order - DEPTH].wait_send()
        if held == OWN:
            merge_piece(piece)
        else:
            receive(held, kind)
        m, row, count = piece
        part = outs[m].at[pl.ds(row, count), columns_of(held)]
        copy = pltpu.make_async_remote_copy(
            src_ref=part,
            dst_ref=part,
            send_sem=send_sems.at[link, order % DEPTH],
            recv_sem=recv_sems.at[seen[0] * 2 + seen[1] - 1, kind],
            device_id=targets[link],
            device_id_type=MESH,
        )
        copy.start()
        sent[link].append(copy)

    col = (z * 2 + xh) * 2 + c
    me = y * 32 + col * 2 + xl
    gain_steps = (
        (answerer, me, 1, targets[2:], greeter),
        (greeter, me // 2 * 2, 2, far_peers[:1], greeter),
        (greeter, me // 4 * 4, 4, far_peers[1:2], greeter),
        (greeter, me // 8 * 8, 8, far_peers[2:], greeter),
        (greeter, y * 32, 32, targets[2:], answerer),
        (None, y * 32, 32, targets[:2], None),
        (None, y_last * 32, 32, targets[:1], None),
    )

    def only(condition, act):
        if condition is None:
            act()
        else:
            pl.when(condition)(act)

    def pass_gains(step):
        if step == 0:
            pltpu.make_async_copy(norms, norms, small_sems.at[2, 0]).wait()
            own_gain[...] = jnp.zeros((1, 1, 128), jnp.float32)
            own_gain[0, :, 0:32] = norms[0] + norms[1]

            @pl.when(greeter)
            def _():
                gains[me] = own_gain[0]

            return
        if step > 1:
            senders, _, count, peers, receivers = gain_steps[step - 2]
            as_many = gains.at[pl.ds(0, count * len(peers))]
            only(senders, pltpu.make_async_copy(as_many, as_many, gain_sends.at[step - 2]).wait)
            only(receivers, pltpu.make_async_copy(as_many, as_many, gain_recvs.at[step - 2]).wait)
        if step == 2:
            only(greeter, lambda: pl.semaphore_wait(barrier, len(far_peers)))
        if step <= len(gain_steps):
            senders, first, count, peers, _ = gain_steps[step - 1]
            part = gains.at[pl.ds(first, count)]

            def start():
                for p in peers:
                    pltpu.make_async_remote_copy(
                        src_ref=own_gain if step == 1 else part,
                        dst_ref=part,
                        send_sem=gain_sends.at[step - 1],
                        recv_sem=gain_recvs.at[step - 1],
                        device_id=p,
                        device_id_type=MESH,
                    ).start()

            only(senders, start)

    @pl.when(answerer)
    def _():
        pl.semaphore_wait(barrier, len(targets))
        for p in targets:
            pl.semaphore_signal(ready, inc=1, device_id=p, device_id_type=MESH)

    merge_piece(kinds[1][0])
    merge_piece(kinds[0][0])

    @pl.when(greeter)
    def _():
        pl.semaphore_wait(ready, len(targets))

    step = 0
    for order, item in enumerate(in_turn(plan_of(kinds))):
        send(*item)
        if order >= 24 and order % 18 == 6 and step <= len(gain_steps) + 1:
            pass_gains(step)
            step += 1

    lane = lax.broadcasted_iota(jnp.int32, (1, 128), 1) // 32
    for r in range(32):
        first = r // 8 * 32 + r % 4 * 8 + r // 4 % 2
        row = gains[first]
        for k in range(1, 4):
            row = jnp.where(lane == k, pltpu.roll(gains[first + 2 * k], 32 * k, 1), row)
        out_norm[r : r + 1, :] = row

    for copies in sent:
        for copy in copies[-DEPTH:]:
            copy.wait_send()
    for oy in range(4):
        for ox in range(2):
            if (oy, ox) != OWN:
                receive((oy, ox), 0)
                receive((oy, ox), 1)


def write_out(gate, up, gain, out_gate, out_up, out_gain, sems):
    step = gate.shape[0] // PARTS
    pairs = ((gate, out_gate), (up, out_up))
    for k in range(PARTS):
        part = pl.ds(k * step, step)
        for m, (source, target) in enumerate(pairs):
            pltpu.make_async_copy(source.at[part], target.at[part], sems.at[m]).start()
    out_gain[...] = gain[...].astype(jnp.bfloat16)
    for m, (source, target) in enumerate(pairs):
        pltpu.make_async_copy(source, target, sems.at[m]).wait()


def per_device(train_gate, low_gate, high_gate, train_up, low_up, high_up, norm_train, norm_step):
    rows, width = train_gate.shape
    whole = rows * 8
    rank = low_gate.shape[1]
    vmem = pl.BlockSpec(memory_space=pltpu.VMEM)
    hbm = pl.BlockSpec(memory_space=pltpu.HBM)
    gathered = pl.pallas_call(
        kernel,
        out_shape=(
            jax.ShapeDtypeStruct((width, whole), jnp.bfloat16),
            jax.ShapeDtypeStruct((width, whole), jnp.bfloat16),
            jax.ShapeDtypeStruct((32, 128), jnp.float32),
        ),
        in_specs=[hbm] * 8,
        out_specs=(vmem, vmem, vmem),
        scratch_shapes=[
            pltpu.VMEM((2, rows, width), jnp.bfloat16),
            pltpu.VMEM((2, rank, rows), jnp.bfloat16),
            pltpu.VMEM((2, rank, width), jnp.bfloat16),
            pltpu.VMEM((2, 1, 32), jnp.float32),
            pltpu.VMEM((1, 1, 128), jnp.float32),
            pltpu.VMEM((128, 1, 128), jnp.float32),
            pltpu.SemaphoreType.DMA((2, len(SPANS))),
            pltpu.SemaphoreType.DMA((3, 2)),
            pltpu.SemaphoreType.DMA((3, DEPTH)),
            pltpu.SemaphoreType.DMA((7, 2)),
            pltpu.SemaphoreType.DMA((7,)),
            pltpu.SemaphoreType.DMA((7,)),
            pltpu.SemaphoreType.REGULAR,
        ],
        compiler_params=pltpu.CompilerParams(
            collective_id=0, has_side_effects=True, vmem_limit_bytes=24 * 1024 * 1024
        ),
        cost_estimate=pl.CostEstimate(flops=10**9, bytes_accessed=2 * 10**7, transcendentals=0),
    )(
        *(
            pltpu.with_memory_space_constraint(x, pltpu.HBM)
            for x in (
                train_gate, low_gate.T, high_gate, train_up, low_up.T, high_up,
                norm_train.reshape(1, 32), norm_step.reshape(1, 32),
            )
        )
    )
    ready_gate, ready_up, gain = pl.pallas_call(
        write_out,
        out_shape=(
            jax.ShapeDtypeStruct((width, whole), jnp.bfloat16),
            jax.ShapeDtypeStruct((width, whole), jnp.bfloat16),
            jax.ShapeDtypeStruct((32, 128), jnp.bfloat16),
        ),
        in_specs=[vmem] * 3,
        out_specs=(hbm, hbm, vmem),
        scratch_shapes=[pltpu.SemaphoreType.DMA((2,))],
        compiler_params=pltpu.CompilerParams(vmem_limit_bytes=24 * 1024 * 1024),
        cost_estimate=pl.CostEstimate(flops=10**7, bytes_accessed=3 * 10**7, transcendentals=0),
    )(*gathered)
    return (ready_gate, ready_up, gain.reshape(-1))


def solution(mesh):
    finer = Mesh(mesh.devices.reshape(SIZES), AXES)
    placed = (
        P(SHARD, COLS),
        P(SHARD, None),
        P(None, COLS),
        P(SHARD, COLS),
        P(SHARD, None),
        P(None, COLS),
        P(SHARD + COLS),
        P(SHARD + COLS),
    )
    return jax.shard_map(
        per_device,
        mesh=finer,
        in_specs=placed,
        out_specs=(P(COLS, None), P(COLS, None), P()),
        check_vma=False,
    )
```

```python
import functools

import jax
import jax.numpy as jnp
from jax import lax
from jax.experimental import pallas as pl
from jax.experimental.pallas import tpu as pltpu
from jax.sharding import Mesh
from jax.sharding import PartitionSpec as P

MESH = pl.DeviceIdType.MESH
AXES = ("y", "xl", "z", "xh", "c")
SHARD = ("y", "xl")
COLS = ("z", "xh", "c")
SIZES = (4, 2, 4, 2, 2)

mix_rate = 1.0

GROUP = 128
CHUNK = 64
SPANS = ((0, 1), (1, 2), (3, 4))
PARTS = 7
DEPTH = 4

OWN, BACK, AHEAD, FAR = (0, 0), (3, 0), (1, 0), (2, 0)


def chunks_of(groups):
    pieces = [(m, g * GROUP + k, CHUNK) for g in range(groups) for m in range(2) for k in range(0, GROUP, CHUNK)]
    kinds = ([], [])
    for k, piece in enumerate(pieces):
        kinds[0 if (k * 5) % 9 < 5 else 1].append(piece)
    m, row, rows = kinds[0].pop()
    kinds[0].append((m, row, rows // 2))
    kinds[1].append((m, row + rows // 2, rows // 2))
    return kinds


def plan_of(kinds):
    first, second = kinds
    up, down, across = [], [], []

    def add(link, held, seen, kind, pieces):
        link.extend((held, seen, kind, piece) for piece in pieces)

    for kind in (1, 0):
        add(up, OWN, BACK, kind, kinds[kind])
        add(down, OWN, AHEAD, kind, kinds[kind])
    add(up, BACK, FAR, 1, second[0::2])
    add(down, AHEAD, FAR, 1, second[1::2])
    add(up, (0, 1), (3, 1), 0, first)
    add(down, (0, 1), (1, 1), 0, first)
    add(up, BACK, FAR, 0, first[0::2])
    add(down, AHEAD, FAR, 0, first[1::2])
    add(up, (3, 1), (2, 1), 0, first[1::2])
    add(down, (1, 1), (2, 1), 0, first[0::2])
    add(across, OWN, (0, 1), 0, first)
    for held in (OWN, BACK, AHEAD, FAR):
        add(across, held, (held[0], 1), 1, second)
    return up, down, across


def in_turn(links):
    places, loads = [0] * len(links), [0] * len(links)
    while any(place < len(link) for place, link in zip(places, links)):
        k = min((loads[k], k) for k in range(len(links)) if places[k] < len(links[k]))[1]
        item = links[k][places[k]]
        yield (k, *item)
        places[k] += 1
        loads[k] += item[-1][2]


def kernel(
    train_gate, low_gate, high_gate, train_up, low_up, high_up, norm_train, norm_step,
    out_gate, out_up, out_norm,
    blocks, lows, highs, norms, gains, packed, load_sems, small_sems, send_sems, recv_sems, gain_sends, gain_recvs, ready,
):
    y, xl, z, xh, c = (lax.axis_index(name) for name in AXES)
    rows, width = train_gate.shape
    groups = width // GROUP
    outs = (out_gate, out_up)

    y_next, y_last = lax.rem(y + 1, 4), lax.rem(y + 3, 4)
    across_x = 1 - xl
    targets = ({"y": y_next}, {"y": y_last}, {"xl": across_x})
    neighbours = ((y_next, xl), (y_last, xl), (y, across_x))

    def at_gate(yy, xx):
        return jnp.logical_and(yy == 1, xx == 0)

    hub_group = jnp.logical_and(xh == 1, c == 1)
    gate = at_gate(y, xl)
    hub = jnp.logical_and(gate, hub_group)
    speaker = jnp.logical_and(gate, jnp.logical_not(hub_group))
    nearby = [jnp.logical_and(hub_group, at_gate(*place)) for place in neighbours]
    other_hubs = [{"z": lax.rem(z + k, 4)} for k in (1, 3, 2)]
    speakers = [{"c": 0}, {"xh": 0}, {"xh": 0, "c": 0}]
    barrier = pltpu.get_barrier_semaphore()

    def greet(sem, *peers):
        for p in peers:
            pl.semaphore_signal(sem, inc=1, device_id=p, device_id_type=MESH)

    for target, is_hub in zip(targets, nearby):
        pl.when(jnp.logical_not(is_hub))(functools.partial(greet, barrier, target))
    pl.when(hub)(functools.partial(greet, barrier, *other_hubs))
    pl.when(speaker)(functools.partial(greet, barrier, {"xh": 1, "c": 1}))

    sources = ((train_gate, low_gate, high_gate), (train_up, low_up, high_up))
    loads = {}
    for s, (first, count) in enumerate(SPANS):
        span = pl.ds(first * GROUP, count * GROUP)
        for m, (train, low, high) in enumerate(sources):
            if s == 0:
                loads[m, "high"] = pltpu.make_async_copy(high, highs.at[m], small_sems.at[m, 0])
                loads[m, "low"] = pltpu.make_async_copy(low, lows.at[m], small_sems.at[m, 1])
                loads[m, "high"].start()
                loads[m, "low"].start()
            loads[m, first] = pltpu.make_async_copy(train.at[:, span], blocks.at[m, :, span], load_sems.at[m, s])
            loads[m, first].start()
    for k, norm in enumerate((norm_train, norm_step)):
        pltpu.make_async_copy(norm, norms.at[k], small_sems.at[2, 0]).start()

    def columns_of(owner):
        column = lax.rem(y + owner[0], 4) * 2 + (across_x if owner[1] else xl)
        return pl.ds(pl.multiple_of(column * rows, rows), rows)

    def merge(m, g):
        if g == 0:
            loads[m, "high"].wait()
            loads[m, "low"].wait()
        if (m, g) in loads:
            loads[m, g].wait()
        span = pl.ds(g * GROUP, GROUP)
        high = highs[m, :, span].astype(jnp.float32).T.astype(jnp.bfloat16)
        product = jnp.dot(high, lows[m], preferred_element_type=jnp.float32)
        latest = blocks[m, :, span].T.astype(jnp.float32) + mix_rate * product
        outs[m][span, columns_of(OWN)] = latest.astype(jnp.bfloat16)

    kinds = chunks_of(groups)
    totals = [sum(piece[2] for piece in pieces) for pieces in kinds]
    merged, arrived = set(), set()
    sent = ([], [], [])

    def merge_piece(piece):
        at = (piece[0], piece[1] // GROUP)
        if at not in merged:
            merged.add(at)
            merge(*at)

    def receive(owner, kind):
        if (owner, kind) not in arrived:
            arrived.add((owner, kind))
            as_many = out_gate.at[pl.ds(0, totals[kind] // 2), pl.ds(0, 2 * rows)]
            sem = recv_sems.at[owner[0] * 2 + owner[1] - 1, kind]
            pltpu.make_async_copy(as_many, as_many, sem).wait()

    def send(link, held, seen, kind, piece):
        order = len(sent[link])
        if order >= DEPTH:
            sent[link][order - DEPTH].wait_send()
        if held == OWN:
            merge_piece(piece)
        else:
            receive(held, kind)
        m, row, count = piece
        part = outs[m].at[pl.ds(row, count), columns_of(held)]
        copy = pltpu.make_async_remote_copy(
            src_ref=part,
            dst_ref=part,
            send_sem=send_sems.at[link, order % DEPTH],
            recv_sem=recv_sems.at[seen[0] * 2 + seen[1] - 1, kind],
            device_id=targets[link],
            device_id_type=MESH,
        )
        copy.start()
        sent[link].append(copy)

    col = (z * 2 + xh) * 2 + c
    me = col * 8 + y * 2 + xl
    gain_steps = (
        (None, gains.at[pl.ds(me, 1)], targets[2:], None, 1),
        (None, gains.at[pl.ds(me // 2 * 2, 2)], targets[:2], None, 4),
        (None, gains.at[pl.ds(col * 8 + y_last * 2, 2)], targets[:1], None, 2),
        (speaker, gains.at[pl.ds(col * 8, 8)], [{"xh": 1, "c": 1}], hub, 24),
        (hub, gains.at[pl.ds(z * 32, 32)], other_hubs, hub, 96),
        (hub, out_norm, speakers, speaker, 16),
        (gate, out_norm, targets[2:], jnp.logical_and(y == 1, xl == 1), 16),
        (y == 1, out_norm, targets[:2], jnp.logical_or(y == 0, y == 2), 16),
        (y == 2, out_norm, targets[:1], y == 3, 16),
    )

    def only(condition, act):
        if condition is None:
            act()
        else:
            pl.when(condition)(act)

    def settle(sem, count):
        as_many = gains.at[pl.ds(0, count)]
        pltpu.make_async_copy(as_many, as_many, sem).wait()

    def pack():
        lane = lax.broadcasted_iota(jnp.int32, (1, 128), 1) // 32
        for r in range(32):
            first = r % 4 * 32 + r // 4
            row = gains[first]
            for k in range(1, 4):
                row = jnp.where(lane == k, pltpu.roll(gains[first + 8 * k], 32 * k, 1), row)
            packed[r : r + 1, :] = row
        out_norm[...] = packed[...].astype(jnp.bfloat16)

    def meet():
        pl.semaphore_wait(barrier, len(other_hubs) + len(speakers))
        greet(ready, *speakers)

    def pass_gains(step):
        if step == 0:
            pltpu.make_async_copy(norms, norms, small_sems.at[2, 0]).wait()
            gains[me] = jnp.zeros((1, 128), jnp.float32)
            gains[me, :, 0:32] = norms[0] + norms[1]
            only(hub, meet)
            return
        if step > 1:
            senders, part, peers, receivers, received = gain_steps[step - 2]
            count = 16 if part is out_norm else part.shape[0]
            only(senders, functools.partial(settle, gain_sends.at[step - 2], count * len(peers)))
            only(receivers, functools.partial(settle, gain_recvs.at[step - 2], received))
        if step <= len(gain_steps):
            senders, part, peers, _, _ = gain_steps[step - 1]

            def start():
                if step == 4:
                    pl.semaphore_wait(ready, 1)
                if step == 6:
                    pack()
                for p in peers:
                    pltpu.make_async_remote_copy(
                        src_ref=part,
                        dst_ref=part,
                        send_sem=gain_sends.at[step - 1],
                        recv_sem=gain_recvs.at[step - 1],
                        device_id=p,
                        device_id_type=MESH,
                    ).start()

            only(senders, start)

    merge_piece(kinds[1][0])
    merge_piece(kinds[0][0])

    @pl.when(hub)
    def _():
        pl.semaphore_wait(ready, len(targets))

    @pl.when(jnp.logical_not(hub))
    def _():
        pl.semaphore_wait(barrier, len(targets))
        for target, is_hub in zip(targets, nearby):
            pl.when(is_hub)(functools.partial(greet, ready, target))

    step = 0
    for order, item in enumerate(in_turn(plan_of(kinds))):
        send(*item)
        if order >= 24 and order % 16 == 8 and step <= len(gain_steps) + 1:
            pass_gains(step)
            step += 1

    for copies in sent:
        for copy in copies[-DEPTH:]:
            copy.wait_send()
    for oy in range(4):
        for ox in range(2):
            if (oy, ox) != OWN:
                receive((oy, ox), 0)
                receive((oy, ox), 1)


def write_out(gate, up, gain, out_gate, out_up, out_gain, sems):
    step = gate.shape[0] // PARTS
    pairs = ((gate, out_gate), (up, out_up))
    for k in range(PARTS):
        part = pl.ds(k * step, step)
        for m, (source, target) in enumerate(pairs):
            pltpu.make_async_copy(source.at[part], target.at[part], sems.at[m]).start()
    out_gain[...] = gain[...]
    for m, (source, target) in enumerate(pairs):
        pltpu.make_async_copy(source, target, sems.at[m]).wait()


def per_device(train_gate, low_gate, high_gate, train_up, low_up, high_up, norm_train, norm_step):
    rows, width = train_gate.shape
    whole = rows * 8
    rank = low_gate.shape[1]
    vmem = pl.BlockSpec(memory_space=pltpu.VMEM)
    hbm = pl.BlockSpec(memory_space=pltpu.HBM)
    gathered = pl.pallas_call(
        kernel,
        out_shape=(
            jax.ShapeDtypeStruct((width, whole), jnp.bfloat16),
            jax.ShapeDtypeStruct((width, whole), jnp.bfloat16),
            jax.ShapeDtypeStruct((32, 128), jnp.bfloat16),
        ),
        in_specs=[hbm] * 8,
        out_specs=(vmem, vmem, vmem),
        scratch_shapes=[
            pltpu.VMEM((2, rows, width), jnp.bfloat16),
            pltpu.VMEM((2, rank, rows), jnp.bfloat16),
            pltpu.VMEM((2, rank, width), jnp.bfloat16),
            pltpu.VMEM((2, 1, 32), jnp.float32),
            pltpu.VMEM((128, 1, 128), jnp.float32),
            pltpu.VMEM((32, 128), jnp.float32),
            pltpu.SemaphoreType.DMA((2, len(SPANS))),
            pltpu.SemaphoreType.DMA((3, 2)),
            pltpu.SemaphoreType.DMA((3, DEPTH)),
            pltpu.SemaphoreType.DMA((7, 2)),
            pltpu.SemaphoreType.DMA((9,)),
            pltpu.SemaphoreType.DMA((9,)),
            pltpu.SemaphoreType.REGULAR,
        ],
        compiler_params=pltpu.CompilerParams(
            collective_id=0, has_side_effects=True, vmem_limit_bytes=24 * 1024 * 1024
        ),
        cost_estimate=pl.CostEstimate(flops=10**9, bytes_accessed=2 * 10**7, transcendentals=0),
    )(
        *(
            pltpu.with_memory_space_constraint(x, pltpu.HBM)
            for x in (
                train_gate, low_gate.T, high_gate, train_up, low_up.T, high_up,
                norm_train.reshape(1, 32), norm_step.reshape(1, 32),
            )
        )
    )
    ready_gate, ready_up, gain = pl.pallas_call(
        write_out,
        out_shape=(
            jax.ShapeDtypeStruct((width, whole), jnp.bfloat16),
            jax.ShapeDtypeStruct((width, whole), jnp.bfloat16),
            jax.ShapeDtypeStruct((32, 128), jnp.bfloat16),
        ),
        in_specs=[vmem] * 3,
        out_specs=(hbm, hbm, vmem),
        scratch_shapes=[pltpu.SemaphoreType.DMA((2,))],
        compiler_params=pltpu.CompilerParams(vmem_limit_bytes=24 * 1024 * 1024),
        cost_estimate=pl.CostEstimate(flops=10**7, bytes_accessed=3 * 10**7, transcendentals=0),
    )(*gathered)
    return (ready_gate, ready_up, gain.reshape(-1))


def solution(mesh):
    finer = Mesh(mesh.devices.reshape(SIZES), AXES)
    placed = (
        P(SHARD, COLS),
        P(SHARD, None),
        P(None, COLS),
        P(SHARD, COLS),
        P(SHARD, None),
        P(None, COLS),
        P(SHARD + COLS),
        P(SHARD + COLS),
    )
    return jax.shard_map(
        per_device,
        mesh=finer,
        in_specs=placed,
        out_specs=(P(COLS, None), P(COLS, None), P()),
        check_vma=False,
    )
```

```python
import functools

import jax
import jax.numpy as jnp
from jax import lax
from jax.experimental import pallas as pl
from jax.experimental.pallas import tpu as pltpu
from jax.sharding import Mesh
from jax.sharding import PartitionSpec as P

MESH = pl.DeviceIdType.MESH
AXES = ("y", "xl", "z", "xh", "c")
SHARD = ("y", "xl")
COLS = ("z", "xh", "c")
SIZES = (4, 2, 4, 2, 2)

mix_rate = 1.0

GROUP = 128
CHUNK = 64
SPANS = ((0, 1), (1, 6))
PARTS = 7
DEPTH = 4

OWN, BACK, AHEAD, FAR = (0, 0), (3, 0), (1, 0), (2, 0)


def chunks_of(groups):
    pieces = [(m, g * GROUP + k, CHUNK) for g in range(groups) for m in range(2) for k in range(0, GROUP, CHUNK)]
    kinds = ([], [])
    for k, piece in enumerate(pieces):
        kinds[0 if (k * 5) % 9 < 5 else 1].append(piece)
    m, row, rows = kinds[0].pop()
    kinds[0].append((m, row, rows // 2))
    kinds[1].append((m, row + rows // 2, rows // 2))
    return kinds


def plan_of(kinds):
    first, second = kinds
    up, down, across = [], [], []

    def add(link, held, seen, kind, pieces):
        link.extend((held, seen, kind, piece) for piece in pieces)

    for kind in (1, 0):
        add(up, OWN, BACK, kind, kinds[kind])
        add(down, OWN, AHEAD, kind, kinds[kind])
    add(up, BACK, FAR, 1, second[0::2])
    add(down, AHEAD, FAR, 1, second[1::2])
    add(up, (0, 1), (3, 1), 0, first)
    add(down, (0, 1), (1, 1), 0, first)
    add(up, BACK, FAR, 0, first[0::2])
    add(down, AHEAD, FAR, 0, first[1::2])
    add(up, (3, 1), (2, 1), 0, first[1::2])
    add(down, (1, 1), (2, 1), 0, first[0::2])
    add(across, OWN, (0, 1), 0, first)
    for held in (OWN, BACK, AHEAD, FAR):
        add(across, held, (held[0], 1), 1, second)
    return up, down, across


def in_turn(links):
    places, loads = [0] * len(links), [0] * len(links)
    while any(place < len(link) for place, link in zip(places, links)):
        k = min((loads[k], k) for k in range(len(links)) if places[k] < len(links[k]))[1]
        item = links[k][places[k]]
        yield (k, *item)
        places[k] += 1
        loads[k] += item[-1][2]


def kernel(
    train_gate, low_gate, high_gate, train_up, low_up, high_up, norm_train, norm_step,
    out_gate, out_up, out_norm,
    blocks, lows, highs, norms, gains, packed, load_sems, small_sems, send_sems, recv_sems, gain_sends, gain_recvs, ready,
):
    y, xl, z, xh, c = (lax.axis_index(name) for name in AXES)
    rows, width = train_gate.shape
    groups = width // GROUP
    outs = (out_gate, out_up)

    y_next, y_last = lax.rem(y + 1, 4), lax.rem(y + 3, 4)
    across_x = 1 - xl
    targets = ({"y": y_next}, {"y": y_last}, {"xl": across_x})
    neighbours = ((y_next, xl), (y_last, xl), (y, across_x))

    def at_gate(yy, xx):
        return jnp.logical_and(yy == 1, xx == 0)

    hub_group = jnp.logical_and(xh == 1, c == 1)
    gate = at_gate(y, xl)
    hub = jnp.logical_and(gate, hub_group)
    speaker = jnp.logical_and(gate, jnp.logical_not(hub_group))
    nearby = [jnp.logical_and(hub_group, at_gate(*place)) for place in neighbours]
    other_hubs = [{"z": lax.rem(z + k, 4)} for k in (1, 3, 2)]
    speakers = [{"c": 0}, {"xh": 0}, {"xh": 0, "c": 0}]
    barrier = pltpu.get_barrier_semaphore()

    def greet(sem, *peers):
        for p in peers:
            pl.semaphore_signal(sem, inc=1, device_id=p, device_id_type=MESH)

    sources = ((train_gate, low_gate, high_gate), (train_up, low_up, high_up))
    loads = {}

    def load(m, s):
        train, low, high = sources[m]
        first, count = SPANS[s]
        span = pl.ds(first * GROUP, count * GROUP)
        started = [pltpu.make_async_copy(train.at[:, span], blocks.at[m, :, span], load_sems.at[m, s])]
        if s == 0:
            started.append(pltpu.make_async_copy(high, highs.at[m], small_sems.at[2 * m]))
            started.append(pltpu.make_async_copy(low, lows.at[m], small_sems.at[2 * m + 1]))
        for copy in started:
            copy.start()
        loads[m, first] = started

    load(0, 0)
    for target, is_hub in zip(targets, nearby):
        pl.when(jnp.logical_not(is_hub))(functools.partial(greet, barrier, target))
    pl.when(hub)(functools.partial(greet, barrier, *other_hubs))
    pl.when(speaker)(functools.partial(greet, barrier, {"xh": 1, "c": 1}))

    for m, s in ((1, 0), (0, 1), (1, 1)):
        load(m, s)
    for k, norm in enumerate((norm_train, norm_step)):
        pltpu.make_async_copy(norm, norms.at[k], small_sems.at[4]).start()

    def columns_of(owner):
        column = lax.rem(y + owner[0], 4) * 2 + (across_x if owner[1] else xl)
        return pl.ds(pl.multiple_of(column * rows, rows), rows)

    def merge(m, g):
        for copy in loads.get((m, g), ()):
            copy.wait()
        span = pl.ds(g * GROUP, GROUP)
        high = highs[m, :, span].astype(jnp.float32).T.astype(jnp.bfloat16)
        product = jnp.dot(high, lows[m], preferred_element_type=jnp.float32)
        latest = blocks[m, :, span].T.astype(jnp.float32) + mix_rate * product
        outs[m][span, columns_of(OWN)] = latest.astype(jnp.bfloat16)

    kinds = chunks_of(groups)
    totals = [sum(piece[2] for piece in pieces) for pieces in kinds]
    merged, arrived = set(), set()
    sent = ([], [], [])

    def merge_piece(piece):
        at = (piece[0], piece[1] // GROUP)
        if at not in merged:
            merged.add(at)
            merge(*at)

    def receive(owner, kind):
        if (owner, kind) not in arrived:
            arrived.add((owner, kind))
            as_many = out_gate.at[pl.ds(0, totals[kind] // 2), pl.ds(0, 2 * rows)]
            sem = recv_sems.at[owner[0] * 2 + owner[1] - 1, kind]
            pltpu.make_async_copy(as_many, as_many, sem).wait()

    def send(link, held, seen, kind, piece):
        order = len(sent[link])
        if order >= DEPTH:
            sent[link][order - DEPTH].wait_send()
        if held == OWN:
            merge_piece(piece)
        else:
            receive(held, kind)
        m, row, count = piece
        part = outs[m].at[pl.ds(row, count), columns_of(held)]
        copy = pltpu.make_async_remote_copy(
            src_ref=part,
            dst_ref=part,
            send_sem=send_sems.at[link, order % DEPTH],
            recv_sem=recv_sems.at[seen[0] * 2 + seen[1] - 1, kind],
            device_id=targets[link],
            device_id_type=MESH,
        )
        copy.start()
        sent[link].append(copy)

    col = (z * 2 + xh) * 2 + c
    me = col * 8 + y * 2 + xl
    gain_steps = (
        (None, gains.at[pl.ds(me, 1)], targets[2:], None, 1),
        (None, gains.at[pl.ds(me // 2 * 2, 2)], targets[:2], None, 4),
        (None, gains.at[pl.ds(col * 8 + y_last * 2, 2)], targets[:1], None, 2),
        (speaker, gains.at[pl.ds(col * 8, 8)], [{"xh": 1, "c": 1}], hub, 24),
        (hub, gains.at[pl.ds(z * 32, 32)], other_hubs, hub, 96),
        (hub, out_norm, speakers, speaker, 16),
        (gate, out_norm, targets[2:], jnp.logical_and(y == 1, xl == 1), 16),
        (y == 1, out_norm, targets[:2], jnp.logical_or(y == 0, y == 2), 16),
        (y == 2, out_norm, targets[:1], y == 3, 16),
    )

    def only(condition, act):
        if condition is None:
            act()
        else:
            pl.when(condition)(act)

    def settle(sem, count):
        as_many = gains.at[pl.ds(0, count)]
        pltpu.make_async_copy(as_many, as_many, sem).wait()

    def pack():
        lane = lax.broadcasted_iota(jnp.int32, (1, 128), 1) // 32
        for r in range(32):
            first = r % 4 * 32 + r // 4
            row = gains[first]
            for k in range(1, 4):
                row = jnp.where(lane == k, pltpu.roll(gains[first + 8 * k], 32 * k, 1), row)
            packed[r : r + 1, :] = row
        out_norm[...] = packed[...].astype(jnp.bfloat16)

    def meet():
        pl.semaphore_wait(barrier, len(other_hubs) + len(speakers))
        greet(ready, *speakers)

    def pass_gains(step):
        if step == 0:
            pltpu.make_async_copy(norms, norms, small_sems.at[4]).wait()
            gains[me] = jnp.zeros((1, 128), jnp.float32)
            gains[me, :, 0:32] = norms[0] + norms[1]
            only(hub, meet)
            return
        if step > 1:
            senders, part, peers, receivers, received = gain_steps[step - 2]
            count = 16 if part is out_norm else part.shape[0]
            only(senders, functools.partial(settle, gain_sends.at[0], count * len(peers)))
            only(receivers, functools.partial(settle, gain_recvs.at[step - 2], received))
        if step <= len(gain_steps):
            senders, part, peers, _, _ = gain_steps[step - 1]

            def start():
                if step == 4:
                    pl.semaphore_wait(ready, 1)
                if step == 6:
                    pack()
                for p in peers:
                    pltpu.make_async_remote_copy(
                        src_ref=part,
                        dst_ref=part,
                        send_sem=gain_sends.at[0],
                        recv_sem=gain_recvs.at[step - 1],
                        device_id=p,
                        device_id_type=MESH,
                    ).start()

            only(senders, start)

    merge_piece(kinds[1][0])
    merge_piece(kinds[0][0])

    @pl.when(hub)
    def _():
        pl.semaphore_wait(ready, len(targets))

    @pl.when(jnp.logical_not(hub))
    def _():
        pl.semaphore_wait(barrier, len(targets))
        for target, is_hub in zip(targets, nearby):
            pl.when(is_hub)(functools.partial(greet, ready, target))

    step = 0
    for order, item in enumerate(in_turn(plan_of(kinds))):
        send(*item)
        if order >= 24 and order % 16 == 8 and step <= len(gain_steps) + 1:
            pass_gains(step)
            step += 1

    for copies in sent:
        for copy in copies[-DEPTH:]:
            copy.wait_send()
    for oy in range(4):
        for ox in range(2):
            if (oy, ox) != OWN:
                receive((oy, ox), 0)
                receive((oy, ox), 1)


def write_out(gate, up, gain, out_gate, out_up, out_gain, sems):
    step = gate.shape[0] // PARTS
    pairs = ((gate, out_gate), (up, out_up))
    for k in range(PARTS):
        part = pl.ds(k * step, step)
        for m, (source, target) in enumerate(pairs):
            pltpu.make_async_copy(source.at[part], target.at[part], sems.at[m]).start()
    small = pltpu.make_async_copy(gain, out_gain, sems.at[2])
    small.start()
    for m, (source, target) in enumerate(pairs):
        pltpu.make_async_copy(source, target, sems.at[m]).wait()
    small.wait()


def per_device(train_gate, low_gate, high_gate, train_up, low_up, high_up, norm_train, norm_step):
    rows, width = train_gate.shape
    whole = rows * 8
    rank = low_gate.shape[1]
    vmem = pl.BlockSpec(memory_space=pltpu.VMEM)
    hbm = pl.BlockSpec(memory_space=pltpu.HBM)
    gathered = pl.pallas_call(
        kernel,
        out_shape=(
            jax.ShapeDtypeStruct((width, whole), jnp.bfloat16),
            jax.ShapeDtypeStruct((width, whole), jnp.bfloat16),
            jax.ShapeDtypeStruct((32, 128), jnp.bfloat16),
        ),
        in_specs=[hbm] * 8,
        out_specs=(vmem, vmem, vmem),
        scratch_shapes=[
            pltpu.VMEM((2, rows, width), jnp.bfloat16),
            pltpu.VMEM((2, rank, rows), jnp.bfloat16),
            pltpu.VMEM((2, rank, width), jnp.bfloat16),
            pltpu.VMEM((2, 1, 32), jnp.float32),
            pltpu.VMEM((128, 1, 128), jnp.float32),
            pltpu.VMEM((32, 128), jnp.float32),
            pltpu.SemaphoreType.DMA((2, len(SPANS))),
            pltpu.SemaphoreType.DMA((5,)),
            pltpu.SemaphoreType.DMA((3, DEPTH)),
            pltpu.SemaphoreType.DMA((7, 2)),
            pltpu.SemaphoreType.DMA((1,)),
            pltpu.SemaphoreType.DMA((9,)),
            pltpu.SemaphoreType.REGULAR,
        ],
        compiler_params=pltpu.CompilerParams(
            collective_id=0, has_side_effects=True, vmem_limit_bytes=24 * 1024 * 1024
        ),
        cost_estimate=pl.CostEstimate(flops=10**9, bytes_accessed=2 * 10**7, transcendentals=0),
    )(
        *(
            pltpu.with_memory_space_constraint(x, pltpu.HBM)
            for x in (
                train_gate, low_gate.T, high_gate, train_up, low_up.T, high_up,
                norm_train.reshape(1, 32), norm_step.reshape(1, 32),
            )
        )
    )
    ready_gate, ready_up, gain = pl.pallas_call(
        write_out,
        out_shape=(
            jax.ShapeDtypeStruct((width, whole), jnp.bfloat16),
            jax.ShapeDtypeStruct((width, whole), jnp.bfloat16),
            jax.ShapeDtypeStruct((32, 128), jnp.bfloat16),
        ),
        in_specs=[vmem] * 3,
        out_specs=(hbm, hbm, hbm),
        scratch_shapes=[pltpu.SemaphoreType.DMA((3,))],
        compiler_params=pltpu.CompilerParams(vmem_limit_bytes=24 * 1024 * 1024),
        cost_estimate=pl.CostEstimate(flops=10**7, bytes_accessed=3 * 10**7, transcendentals=0),
    )(*gathered)
    return (ready_gate, ready_up, gain.reshape(-1))


def solution(mesh):
    finer = Mesh(mesh.devices.reshape(SIZES), AXES)
    placed = (
        P(SHARD, COLS),
        P(SHARD, None),
        P(None, COLS),
        P(SHARD, COLS),
        P(SHARD, None),
        P(None, COLS),
        P(SHARD + COLS),
        P(SHARD + COLS),
    )
    return jax.shard_map(
        per_device,
        mesh=finer,
        in_specs=placed,
        out_specs=(P(COLS, None), P(COLS, None), P()),
        check_vma=False,
    )
```

```python
import functools

import jax
import jax.numpy as jnp
from jax import lax
from jax.experimental import pallas as pl
from jax.experimental.pallas import tpu as pltpu
from jax.sharding import Mesh
from jax.sharding import PartitionSpec as P

MESH = pl.DeviceIdType.MESH
AXES = ("y", "xl", "z", "xh", "c")
SHARD = ("y", "xl")
COLS = ("z", "xh", "c")
SIZES = (4, 2, 4, 2, 2)

mix_rate = 1.0

GROUP = 128
CHUNK = 64
PARTS = 4
DEPTH = 4
FIRST = (9, 12)
GAIN_EVERY = 8

OWN, BACK, AHEAD, FAR = (0, 0), (3, 0), (1, 0), (2, 0)


def shares_of(groups):
    every = [(m, g) for g in range(groups) for m in range(2)]
    return [(every[:count], every[count:]) for count in FIRST]


def chunks_of(share):
    pieces = [(m, g * GROUP + k, CHUNK) for m, g in share for k in range(0, GROUP, CHUNK)]
    kinds = ([], [])
    for k, piece in enumerate(pieces):
        kinds[0 if (k * 5) % 9 < 5 else 1].append(piece)
    excess = sum(piece[2] for piece in kinds[0]) - (len(share) * GROUP * 5 + 72) // 144 * 16
    if excess:
        giver, taker = kinds if excess > 0 else kinds[::-1]
        m, row, rows = giver.pop()
        giver.append((m, row, rows - abs(excess)))
        taker.append((m, row + rows - abs(excess), abs(excess)))
    return kinds


def plan_of(kinds):
    first, second = kinds
    up, down, across = [], [], []

    def add(link, held, seen, kind, pieces):
        link.extend((held, seen, kind, piece) for piece in pieces)

    for kind in (1, 0):
        add(up, OWN, BACK, kind, kinds[kind])
        add(down, OWN, AHEAD, kind, kinds[kind])
    add(up, BACK, FAR, 1, second[0::2])
    add(down, AHEAD, FAR, 1, second[1::2])
    add(up, (0, 1), (3, 1), 0, first)
    add(down, (0, 1), (1, 1), 0, first)
    add(up, BACK, FAR, 0, first[0::2])
    add(down, AHEAD, FAR, 0, first[1::2])
    add(up, (3, 1), (2, 1), 0, first[1::2])
    add(down, (1, 1), (2, 1), 0, first[0::2])
    add(across, OWN, (0, 1), 0, first)
    for held in (OWN, BACK, AHEAD, FAR):
        add(across, held, (held[0], 1), 1, second)
    return up, down, across


def in_turn(links):
    places, loads = [0] * len(links), [0] * len(links)
    while any(place < len(link) for place, link in zip(places, links)):
        k = min((loads[k], k) for k in range(len(links)) if places[k] < len(links[k]))[1]
        item = links[k][places[k]]
        yield (k, *item)
        places[k] += 1
        loads[k] += item[-1][2]


def greet(sem, *peers):
    for p in peers:
        pl.semaphore_signal(sem, inc=1, device_id=p, device_id_type=MESH)


def only(condition, act):
    if condition is None:
        act()
    else:
        pl.when(condition)(act)


def pass_rows(shares, sources, window, blocks, lows, highs, load_sems, small_sems, send_sems, recv_sems, enter, between):
    y, xl, c = (lax.axis_index(name) for name in ("y", "xl", "c"))
    rows = sources[0][0].shape[0]
    across_x = 1 - xl
    targets = ({"y": lax.rem(y + 1, 4)}, {"y": lax.rem(y + 3, 4)}, {"xl": across_x})

    def columns_of(owner):
        column = lax.rem(y + owner[0], 4) * 2 + (across_x if owner[1] else xl)
        return pl.ds(pl.multiple_of(column * rows, rows), rows)

    def run(core, share):
        loads = {}

        def load(m, groups, sem, small):
            train, low, high = sources[m]
            span = pl.ds(groups[0] * GROUP, len(groups) * GROUP)
            started = [pltpu.make_async_copy(train.at[:, span], blocks.at[m, :, span], load_sems.at[m, sem])]
            if small:
                started.append(pltpu.make_async_copy(high, highs.at[m], small_sems.at[2 * m]))
                started.append(pltpu.make_async_copy(low, lows.at[m], small_sems.at[2 * m + 1]))
            for copy in started:
                copy.start()
            loads[m, groups[0]] = started

        mine = [[g for m, g in share if m == k] for k in range(2)]
        order = (share[0][0], 1 - share[0][0])
        for m in order:
            if mine[m]:
                load(m, mine[m][:1], 0, True)
        for m in order:
            if mine[m][1:]:
                load(m, mine[m][1:], 1, False)

        def merge(m, g):
            for copy in loads.get((m, g), ()):
                copy.wait()
            span = pl.ds(g * GROUP, GROUP)
            high = highs[m, :, span].astype(jnp.float32).T.astype(jnp.bfloat16)
            product = jnp.dot(high, lows[m], preferred_element_type=jnp.float32)
            latest = blocks[m, :, span].T.astype(jnp.float32) + mix_rate * product
            ref, row = window(share, m, g * GROUP)
            ref[pl.ds(row, GROUP), columns_of(OWN)] = latest.astype(jnp.bfloat16)

        kinds = chunks_of(share)
        totals = [sum(piece[2] for piece in pieces) for pieces in kinds]
        merged, arrived = set(), set()
        sent = ([], [], [])

        def merge_piece(piece):
            at = (piece[0], piece[1] // GROUP)
            if at not in merged:
                merged.add(at)
                merge(*at)

        def receive(owner, kind):
            if (owner, kind) not in arrived:
                arrived.add((owner, kind))
                as_many = window(share, share[0][0], share[0][1] * GROUP)[0].at[pl.ds(0, totals[kind] // 2), pl.ds(0, 2 * rows)]
                sem = recv_sems.at[owner[0] * 2 + owner[1] - 1, kind]
                pltpu.make_async_copy(as_many, as_many, sem).wait()

        def send(link, held, seen, kind, piece):
            order = len(sent[link])
            if order >= DEPTH:
                sent[link][order - DEPTH].wait_send()
            if held == OWN:
                merge_piece(piece)
            else:
                receive(held, kind)
            m, row, count = piece
            ref, row = window(share, m, row)
            part = ref.at[pl.ds(row, count), columns_of(held)]
            copy = pltpu.make_async_remote_copy(
                src_ref=part,
                dst_ref=part,
                send_sem=send_sems.at[link, order % DEPTH],
                recv_sem=recv_sems.at[seen[0] * 2 + seen[1] - 1, kind],
                device_id=targets[link],
                device_id_type=MESH,
            )
            copy.start()
            sent[link].append(copy)

        merge_piece(kinds[1][0])
        merge_piece(kinds[0][0])
        enter(targets)
        for order, item in enumerate(in_turn(plan_of(kinds))):
            send(*item)
            between(order)
        for copies in sent:
            for copy in copies[-DEPTH:]:
                copy.wait_send()
        for oy in range(4):
            for ox in range(2):
                if (oy, ox) != OWN:
                    receive((oy, ox), 0)
                    receive((oy, ox), 1)

    for core, share in enumerate(shares):
        pl.when(c == core)(functools.partial(run, core, share))


def first_kernel(
    train_gate, low_gate, high_gate, train_up, low_up, high_up, norm_train, norm_step,
    out_gate, out_up, out_norm,
    blocks, lows, highs, load_sems, small_sems, send_sems, recv_sems,
    norms, gains, packed, gain_sends, gain_recvs, ready,
):
    y, xl, z, xh, c = (lax.axis_index(name) for name in AXES)
    y_next, y_last = lax.rem(y + 1, 4), lax.rem(y + 3, 4)
    across_x = 1 - xl
    targets = ({"y": y_next}, {"y": y_last}, {"xl": across_x})
    neighbours = ((y_next, xl), (y_last, xl), (y, across_x))

    def at_gate(yy, xx):
        return jnp.logical_and(yy == 1, xx == 0)

    hub_group = jnp.logical_and(xh == 1, c == 1)
    gate = at_gate(y, xl)
    hub = jnp.logical_and(gate, hub_group)
    speaker = jnp.logical_and(gate, jnp.logical_not(hub_group))
    nearby = [jnp.logical_and(hub_group, at_gate(*place)) for place in neighbours]
    other_hubs = [{"z": lax.rem(z + k, 4)} for k in (1, 3, 2)]
    speakers = [{"c": 0}, {"xh": 0}, {"xh": 0, "c": 0}]
    barrier = pltpu.get_barrier_semaphore()

    for target, is_hub in zip(targets, nearby):
        pl.when(jnp.logical_not(is_hub))(functools.partial(greet, barrier, target))
    pl.when(hub)(functools.partial(greet, barrier, *other_hubs))
    pl.when(speaker)(functools.partial(greet, barrier, {"xh": 1, "c": 1}))
    for k, norm in enumerate((norm_train, norm_step)):
        pltpu.make_async_copy(norm, norms.at[k], small_sems.at[4]).start()

    def enter(targets):
        @pl.when(hub)
        def _():
            pl.semaphore_wait(ready, len(targets))

        @pl.when(jnp.logical_not(hub))
        def _():
            pl.semaphore_wait(barrier, len(targets))
            for target, is_hub in zip(targets, nearby):
                pl.when(is_hub)(functools.partial(greet, ready, target))

    col = (z * 2 + xh) * 2 + c
    me = col * 8 + y * 2 + xl
    gain_steps = (
        (None, gains.at[pl.ds(me, 1)], targets[2:], None, 1),
        (None, gains.at[pl.ds(me // 2 * 2, 2)], targets[:2], None, 4),
        (None, gains.at[pl.ds(col * 8 + y_last * 2, 2)], targets[:1], None, 2),
        (speaker, gains.at[pl.ds(col * 8, 8)], [{"xh": 1, "c": 1}], hub, 24),
        (hub, gains.at[pl.ds(z * 32, 32)], other_hubs, hub, 96),
        (hub, out_norm, speakers, speaker, 16),
        (gate, out_norm, targets[2:], jnp.logical_and(y == 1, xl == 1), 16),
        (y == 1, out_norm, targets[:2], jnp.logical_or(y == 0, y == 2), 16),
        (y == 2, out_norm, targets[:1], y == 3, 16),
    )

    def settle(sem, count):
        as_many = gains.at[pl.ds(0, count)]
        pltpu.make_async_copy(as_many, as_many, sem).wait()

    def pack():
        lane = lax.broadcasted_iota(jnp.int32, (1, 128), 1) // 32
        for r in range(32):
            first = r % 4 * 32 + r // 4
            row = gains[first]
            for k in range(1, 4):
                row = jnp.where(lane == k, pltpu.roll(gains[first + 8 * k], 32 * k, 1), row)
            packed[r : r + 1, :] = row
        out_norm[...] = packed[...].astype(jnp.bfloat16)

    def meet():
        pl.semaphore_wait(barrier, len(other_hubs) + len(speakers))
        greet(ready, *speakers)

    def pass_gains(step):
        if step == 0:
            pltpu.make_async_copy(norms, norms, small_sems.at[4]).wait()
            gains[me] = jnp.zeros((1, 128), jnp.float32)
            gains[me, :, 0:32] = norms[0] + norms[1]
            only(hub, meet)
            return
        if step > 1:
            senders, part, peers, receivers, received = gain_steps[step - 2]
            count = 16 if part is out_norm else part.shape[0]
            only(senders, functools.partial(settle, gain_sends.at[0], count * len(peers)))
            only(receivers, functools.partial(settle, gain_recvs.at[step - 2], received))
        if step <= len(gain_steps):
            senders, part, peers, _, _ = gain_steps[step - 1]

            def start():
                if step == 4:
                    pl.semaphore_wait(ready, 1)
                if step == 6:
                    pack()
                for p in peers:
                    pltpu.make_async_remote_copy(
                        src_ref=part,
                        dst_ref=part,
                        send_sem=gain_sends.at[0],
                        recv_sem=gain_recvs.at[step - 1],
                        device_id=p,
                        device_id_type=MESH,
                    ).start()

            only(senders, start)

    def between(order):
        step, rest = divmod(order - 24, GAIN_EVERY)
        if step >= 0 and rest == 0 and step <= len(gain_steps) + 1:
            pass_gains(step)

    outs = (out_gate, out_up)
    pass_rows(
        [first for first, _ in shares_of(train_gate.shape[1] // GROUP)],
        ((train_gate, low_gate, high_gate), (train_up, low_up, high_up)),
        lambda share, m, row: (outs[m], row),
        blocks, lows, highs, load_sems, small_sems, send_sems, recv_sems, enter, between,
    )


def second_kernel(
    train_gate, low_gate, high_gate, train_up, low_up, high_up, after,
    out,
    blocks, lows, highs, load_sems, small_sems, send_sems, recv_sems,
):
    y, xl = lax.axis_index("y"), lax.axis_index("xl")
    barrier = pltpu.get_barrier_semaphore()
    greet(barrier, {"y": lax.rem(y + 1, 4)}, {"y": lax.rem(y + 3, 4)}, {"xl": 1 - xl})
    pass_rows(
        [second for _, second in shares_of(train_gate.shape[1] // GROUP)],
        ((train_gate, low_gate, high_gate), (train_up, low_up, high_up)),
        lambda share, m, row: (out, share.index((m, row // GROUP)) * GROUP + row % GROUP),
        blocks, lows, highs, load_sems, small_sems, send_sems, recv_sems,
        lambda targets: pl.semaphore_wait(barrier, len(targets)),
        lambda order: None,
    )


def write_first(gate, up, gain, out_gate, out_up, out_gain, sems):
    shares = shares_of(gate.shape[0] // GROUP)
    small = pltpu.make_async_copy(gain, out_gain, sems.at[2])
    small.start()

    def run(share):
        pairs = ((gate, out_gate), (up, out_up))
        ends = [GROUP * sum(m == k for m, _ in share) for k in range(2)]
        for k in range(PARTS):
            for m, (source, target) in enumerate(pairs):
                first, last = (ends[m] // GROUP * n // PARTS * GROUP for n in (k, k + 1))
                if last > first:
                    part = pl.ds(first, last - first)
                    pltpu.make_async_copy(source.at[part], target.at[part], sems.at[m]).start()
        for m, (source, target) in enumerate(pairs):
            part = pl.ds(0, ends[m])
            pltpu.make_async_copy(source.at[part], target.at[part], sems.at[m]).wait()

    for core, (share, _) in enumerate(shares):
        pl.when(lax.axis_index("c") == core)(functools.partial(run, share))
    small.wait()


def write_second(rest, held_gate, held_up, out_gate, out_up, sems):
    shares = shares_of(out_gate.shape[0] // GROUP)

    def run(share):
        copies = []
        for k, (m, g) in enumerate(share):
            source = rest.at[pl.ds(k * GROUP, GROUP)]
            target = (out_gate, out_up)[m].at[pl.ds(g * GROUP, GROUP)]
            copies.append(pltpu.make_async_copy(source, target, sems.at[k]))
            copies[-1].start()
        for copy in copies:
            copy.wait()

    for core, (_, share) in enumerate(shares):
        pl.when(lax.axis_index("c") == core)(functools.partial(run, share))


def per_device(train_gate, low_gate, high_gate, train_up, low_up, high_up, norm_train, norm_step):
    rows, width = train_gate.shape
    whole = rows * 8
    rank = low_gate.shape[1]
    most = max(2 * width // GROUP - count for count in FIRST)
    vmem = pl.BlockSpec(memory_space=pltpu.VMEM)
    hbm = pl.BlockSpec(memory_space=pltpu.HBM)
    matrix = jax.ShapeDtypeStruct((width, whole), jnp.bfloat16)
    gain = jax.ShapeDtypeStruct((32, 128), jnp.bfloat16)
    sources = [
        pltpu.with_memory_space_constraint(x, pltpu.HBM)
        for x in (
            train_gate, low_gate.T, high_gate, train_up, low_up.T, high_up,
            norm_train.reshape(1, 32), norm_step.reshape(1, 32),
        )
    ]
    scratch = [
        pltpu.VMEM((2, rows, width), jnp.bfloat16),
        pltpu.VMEM((2, rank, rows), jnp.bfloat16),
        pltpu.VMEM((2, rank, width), jnp.bfloat16),
        pltpu.SemaphoreType.DMA((2, 2)),
        pltpu.SemaphoreType.DMA((5,)),
        pltpu.SemaphoreType.DMA((3, DEPTH)),
        pltpu.SemaphoreType.DMA((7, 2)),
    ]
    limit = 12 * 1024 * 1024
    gathered = pl.pallas_call(
        first_kernel,
        out_shape=(matrix, matrix, gain),
        in_specs=[hbm] * 8,
        out_specs=(vmem, vmem, vmem),
        scratch_shapes=scratch
        + [
            pltpu.VMEM((2, 1, 32), jnp.float32),
            pltpu.VMEM((128, 1, 128), jnp.float32),
            pltpu.VMEM((32, 128), jnp.float32),
            pltpu.SemaphoreType.DMA((1,)),
            pltpu.SemaphoreType.DMA((9,)),
            pltpu.SemaphoreType.REGULAR,
        ],
        compiler_params=pltpu.CompilerParams(collective_id=0, has_side_effects=True, vmem_limit_bytes=limit),
        cost_estimate=pl.CostEstimate(flops=10**9, bytes_accessed=2 * 10**7, transcendentals=0),
    )(*sources)
    held_gate, held_up, served = pl.pallas_call(
        write_first,
        out_shape=(matrix, matrix, gain),
        in_specs=[vmem] * 3,
        out_specs=(hbm, hbm, hbm),
        scratch_shapes=[pltpu.SemaphoreType.DMA((3,))],
        compiler_params=pltpu.CompilerParams(vmem_limit_bytes=limit),
        cost_estimate=pl.CostEstimate(flops=10**7, bytes_accessed=3 * 10**7, transcendentals=0),
    )(*gathered)
    rest = pl.pallas_call(
        second_kernel,
        out_shape=jax.ShapeDtypeStruct((most * GROUP, whole), jnp.bfloat16),
        in_specs=[hbm] * 7,
        out_specs=vmem,
        scratch_shapes=scratch,
        compiler_params=pltpu.CompilerParams(collective_id=1, has_side_effects=True, vmem_limit_bytes=limit),
        cost_estimate=pl.CostEstimate(flops=10**9, bytes_accessed=2 * 10**7, transcendentals=0),
    )(*sources[:6], pltpu.with_memory_space_constraint(served, pltpu.HBM))
    ready_gate, ready_up = pl.pallas_call(
        write_second,
        out_shape=(matrix, matrix),
        in_specs=[vmem, hbm, hbm],
        out_specs=(hbm, hbm),
        input_output_aliases={1: 0, 2: 1},
        scratch_shapes=[pltpu.SemaphoreType.DMA((most,))],
        compiler_params=pltpu.CompilerParams(vmem_limit_bytes=limit),
        cost_estimate=pl.CostEstimate(flops=10**7, bytes_accessed=10**7, transcendentals=0),
    )(rest, held_gate, held_up)
    return (ready_gate, ready_up, served.reshape(-1))


def solution(mesh):
    finer = Mesh(mesh.devices.reshape(SIZES), AXES)
    placed = (
        P(SHARD, COLS),
        P(SHARD, None),
        P(None, COLS),
        P(SHARD, COLS),
        P(SHARD, None),
        P(None, COLS),
        P(SHARD + COLS),
        P(SHARD + COLS),
    )
    return jax.shard_map(
        per_device,
        mesh=finer,
        in_specs=placed,
        out_specs=(P(COLS, None), P(COLS, None), P()),
        check_vma=False,
    )
```

```python
import functools

import jax
import jax.numpy as jnp
from jax import lax
from jax.experimental import pallas as pl
from jax.experimental.pallas import tpu as pltpu
from jax.sharding import Mesh
from jax.sharding import PartitionSpec as P

MESH = pl.DeviceIdType.MESH
AXES = ("y", "xl", "z", "xh", "c")
SHARD = ("y", "xl")
COLS = ("z", "xh", "c")
SIZES = (4, 2, 4, 2, 2)

mix_rate = 1.0

GROUP = 128
CHUNK = 64
PARTS = 4
DEPTH = 6
FIRST = (9, 12)
GAIN_EVERY = 8

OWN, BACK, AHEAD, FAR = (0, 0), (3, 0), (1, 0), (2, 0)


def shares_of(groups):
    every = [(m, g) for g in range(groups) for m in range(2)]
    return [(every[:count], every[count:]) for count in FIRST]


def chunks_of(share):
    pieces = [(m, g * GROUP + k, CHUNK) for m, g in share for k in range(0, GROUP, CHUNK)]
    kinds = ([], [])
    for k, piece in enumerate(pieces):
        kinds[0 if (k * 5) % 9 < 5 else 1].append(piece)
    excess = sum(piece[2] for piece in kinds[0]) - (len(share) * GROUP * 5 + 72) // 144 * 16
    if excess:
        giver, taker = kinds if excess > 0 else kinds[::-1]
        m, row, rows = giver.pop()
        giver.append((m, row, rows - abs(excess)))
        taker.append((m, row + rows - abs(excess), abs(excess)))
    return kinds


def plan_of(kinds):
    first, second = kinds
    up, down, across = [], [], []

    def add(link, held, seen, kind, pieces):
        link.extend((held, seen, kind, piece) for piece in pieces)

    for kind in (1, 0):
        add(up, OWN, BACK, kind, kinds[kind])
        add(down, OWN, AHEAD, kind, kinds[kind])
    add(up, BACK, FAR, 1, second[0::2])
    add(down, AHEAD, FAR, 1, second[1::2])
    add(up, (0, 1), (3, 1), 0, first)
    add(down, (0, 1), (1, 1), 0, first)
    add(up, BACK, FAR, 0, first[0::2])
    add(down, AHEAD, FAR, 0, first[1::2])
    add(up, (3, 1), (2, 1), 0, first[1::2])
    add(down, (1, 1), (2, 1), 0, first[0::2])
    add(across, OWN, (0, 1), 0, first)
    for held in (OWN, BACK, AHEAD, FAR):
        add(across, held, (held[0], 1), 1, second)
    return up, down, across


def in_turn(links):
    places, loads = [0] * len(links), [0] * len(links)
    while any(place < len(link) for place, link in zip(places, links)):
        k = min((loads[k], k) for k in range(len(links)) if places[k] < len(links[k]))[1]
        item = links[k][places[k]]
        yield (k, *item)
        places[k] += 1
        loads[k] += item[-1][2]


def greet(sem, *peers):
    for p in peers:
        pl.semaphore_signal(sem, inc=1, device_id=p, device_id_type=MESH)


def only(condition, act):
    if condition is None:
        act()
    else:
        pl.when(condition)(act)


def pass_rows(shares, sources, window, blocks, lows, highs, load_sems, small_sems, send_sems, recv_sems, enter, between):
    y, xl, c = (lax.axis_index(name) for name in ("y", "xl", "c"))
    rows = sources[0][0].shape[0]
    across_x = 1 - xl
    targets = ({"y": lax.rem(y + 1, 4)}, {"y": lax.rem(y + 3, 4)}, {"xl": across_x})

    def columns_of(owner):
        column = lax.rem(y + owner[0], 4) * 2 + (across_x if owner[1] else xl)
        return pl.ds(pl.multiple_of(column * rows, rows), rows)

    def run(core, share):
        loads = {}

        def load(m, groups, sem, small):
            train, low, high = sources[m]
            span = pl.ds(groups[0] * GROUP, len(groups) * GROUP)
            started = [pltpu.make_async_copy(train.at[:, span], blocks.at[m, :, span], load_sems.at[m, sem])]
            if small:
                started.append(pltpu.make_async_copy(high, highs.at[m], small_sems.at[2 * m]))
                started.append(pltpu.make_async_copy(low, lows.at[m], small_sems.at[2 * m + 1]))
            for copy in started:
                copy.start()
            loads[m, groups[0]] = started

        mine = [[g for m, g in share if m == k] for k in range(2)]
        order = (share[0][0], 1 - share[0][0])
        for m in order:
            if mine[m]:
                load(m, mine[m][:1], 0, True)
        for m in order:
            if mine[m][1:]:
                load(m, mine[m][1:], 1, False)

        def merge(m, g):
            for copy in loads.get((m, g), ()):
                copy.wait()
            span = pl.ds(g * GROUP, GROUP)
            high = highs[m, :, span].astype(jnp.float32).T.astype(jnp.bfloat16)
            product = jnp.dot(high, lows[m], preferred_element_type=jnp.float32)
            latest = blocks[m, :, span].T.astype(jnp.float32) + mix_rate * product
            ref, row = window(share, m, g * GROUP)
            ref[pl.ds(row, GROUP), columns_of(OWN)] = latest.astype(jnp.bfloat16)

        kinds = chunks_of(share)
        totals = [sum(piece[2] for piece in pieces) for pieces in kinds]
        merged, arrived = set(), set()
        sent = ([], [], [])

        def merge_piece(piece):
            at = (piece[0], piece[1] // GROUP)
            if at not in merged:
                merged.add(at)
                merge(*at)

        def merge_next():
            at = next(at for at in share if at not in merged)
            merged.add(at)
            merge(*at)

        def receive(owner, kind):
            if (owner, kind) not in arrived:
                arrived.add((owner, kind))
                as_many = window(share, share[0][0], share[0][1] * GROUP)[0].at[pl.ds(0, totals[kind] // 2), pl.ds(0, 2 * rows)]
                sem = recv_sems.at[owner[0] * 2 + owner[1] - 1, kind]
                pltpu.make_async_copy(as_many, as_many, sem).wait()

        def send(link, held, seen, kind, piece):
            order = len(sent[link])
            if order >= DEPTH:
                sent[link][order - DEPTH].wait_send()
            if held == OWN:
                merge_piece(piece)
            else:
                receive(held, kind)
            m, row, count = piece
            ref, row = window(share, m, row)
            part = ref.at[pl.ds(row, count), columns_of(held)]
            copy = pltpu.make_async_remote_copy(
                src_ref=part,
                dst_ref=part,
                send_sem=send_sems.at[link, order % DEPTH],
                recv_sem=recv_sems.at[seen[0] * 2 + seen[1] - 1, kind],
                device_id=targets[link],
                device_id_type=MESH,
            )
            copy.start()
            sent[link].append(copy)

        merge_piece(kinds[1][0])
        merge_piece(kinds[0][0])
        enter(targets)
        for order, item in enumerate(in_turn(plan_of(kinds))):
            send(*item)
            if order % 3 == 2 and len(merged) < len(share):
                merge_next()
            between(order)
        for copies in sent:
            for copy in copies[-DEPTH:]:
                copy.wait_send()
        for oy in range(4):
            for ox in range(2):
                if (oy, ox) != OWN:
                    receive((oy, ox), 0)
                    receive((oy, ox), 1)

    for core, share in enumerate(shares):
        pl.when(c == core)(functools.partial(run, core, share))


def first_kernel(
    train_gate, low_gate, high_gate, train_up, low_up, high_up, norm_train, norm_step,
    out_gate, out_up, out_norm,
    blocks, lows, highs, load_sems, small_sems, send_sems, recv_sems,
    norms, gains, packed, gain_sends, gain_recvs, ready,
):
    y, xl, z, xh, c = (lax.axis_index(name) for name in AXES)
    y_next, y_last = lax.rem(y + 1, 4), lax.rem(y + 3, 4)
    across_x = 1 - xl
    targets = ({"y": y_next}, {"y": y_last}, {"xl": across_x})
    neighbours = ((y_next, xl), (y_last, xl), (y, across_x))

    def at_gate(yy, xx):
        return jnp.logical_and(yy == 1, xx == 0)

    hub_group = jnp.logical_and(xh == 1, c == 1)
    gate = at_gate(y, xl)
    hub = jnp.logical_and(gate, hub_group)
    speaker = jnp.logical_and(gate, jnp.logical_not(hub_group))
    nearby = [jnp.logical_and(hub_group, at_gate(*place)) for place in neighbours]
    other_hubs = [{"z": lax.rem(z + k, 4)} for k in (1, 3, 2)]
    speakers = [{"c": 0}, {"xh": 0}, {"xh": 0, "c": 0}]
    barrier = pltpu.get_barrier_semaphore()

    for target, is_hub in zip(targets, nearby):
        pl.when(jnp.logical_not(is_hub))(functools.partial(greet, barrier, target))
    pl.when(hub)(functools.partial(greet, barrier, *other_hubs))
    pl.when(speaker)(functools.partial(greet, barrier, {"xh": 1, "c": 1}))
    for k, norm in enumerate((norm_train, norm_step)):
        pltpu.make_async_copy(norm, norms.at[k], small_sems.at[4]).start()

    def enter(targets):
        @pl.when(hub)
        def _():
            pl.semaphore_wait(ready, len(targets))

        @pl.when(jnp.logical_not(hub))
        def _():
            pl.semaphore_wait(barrier, len(targets))
            for target, is_hub in zip(targets, nearby):
                pl.when(is_hub)(functools.partial(greet, ready, target))

    col = (z * 2 + xh) * 2 + c
    me = col * 8 + y * 2 + xl
    gain_steps = (
        (None, gains.at[pl.ds(me, 1)], targets[2:], None, 1),
        (None, gains.at[pl.ds(me // 2 * 2, 2)], targets[:2], None, 4),
        (None, gains.at[pl.ds(col * 8 + y_last * 2, 2)], targets[:1], None, 2),
        (speaker, gains.at[pl.ds(col * 8, 8)], [{"xh": 1, "c": 1}], hub, 24),
        (hub, gains.at[pl.ds(z * 32, 32)], other_hubs, hub, 96),
        (hub, out_norm, speakers, speaker, 16),
        (gate, out_norm, targets[2:], jnp.logical_and(y == 1, xl == 1), 16),
        (y == 1, out_norm, targets[:2], jnp.logical_or(y == 0, y == 2), 16),
        (y == 2, out_norm, targets[:1], y == 3, 16),
    )

    def settle(sem, count):
        as_many = gains.at[pl.ds(0, count)]
        pltpu.make_async_copy(as_many, as_many, sem).wait()

    def pack():
        lane = lax.broadcasted_iota(jnp.int32, (1, 128), 1) // 32
        for r in range(32):
            first = r % 4 * 32 + r // 4
            row = gains[first]
            for k in range(1, 4):
                row = jnp.where(lane == k, pltpu.roll(gains[first + 8 * k], 32 * k, 1), row)
            packed[r : r + 1, :] = row
        out_norm[...] = packed[...].astype(jnp.bfloat16)

    def meet():
        pl.semaphore_wait(barrier, len(other_hubs) + len(speakers))
        greet(ready, *speakers)

    def pass_gains(step):
        if step == 0:
            pltpu.make_async_copy(norms, norms, small_sems.at[4]).wait()
            gains[me] = jnp.zeros((1, 128), jnp.float32)
            gains[me, :, 0:32] = norms[0] + norms[1]
            only(hub, meet)
            return
        if step > 1:
            senders, part, peers, receivers, received = gain_steps[step - 2]
            count = 16 if part is out_norm else part.shape[0]
            only(senders, functools.partial(settle, gain_sends.at[0], count * len(peers)))
            only(receivers, functools.partial(settle, gain_recvs.at[step - 2], received))
        if step <= len(gain_steps):
            senders, part, peers, _, _ = gain_steps[step - 1]

            def start():
                if step == 4:
                    pl.semaphore_wait(ready, 1)
                if step == 6:
                    pack()
                for p in peers:
                    pltpu.make_async_remote_copy(
                        src_ref=part,
                        dst_ref=part,
                        send_sem=gain_sends.at[0],
                        recv_sem=gain_recvs.at[step - 1],
                        device_id=p,
                        device_id_type=MESH,
                    ).start()

            only(senders, start)

    def between(order):
        step, rest = divmod(order - 24, GAIN_EVERY)
        if step >= 0 and rest == 0 and step <= len(gain_steps) + 1:
            pass_gains(step)

    outs = (out_gate, out_up)
    pass_rows(
        [first for first, _ in shares_of(train_gate.shape[1] // GROUP)],
        ((train_gate, low_gate, high_gate), (train_up, low_up, high_up)),
        lambda share, m, row: (outs[m], row),
        blocks, lows, highs, load_sems, small_sems, send_sems, recv_sems, enter, between,
    )


def second_kernel(
    train_gate, low_gate, high_gate, train_up, low_up, high_up, after,
    out,
    blocks, lows, highs, load_sems, small_sems, send_sems, recv_sems,
):
    y, xl = lax.axis_index("y"), lax.axis_index("xl")
    barrier = pltpu.get_barrier_semaphore()
    greet(barrier, {"y": lax.rem(y + 1, 4)}, {"y": lax.rem(y + 3, 4)}, {"xl": 1 - xl})
    pass_rows(
        [second for _, second in shares_of(train_gate.shape[1] // GROUP)],
        ((train_gate, low_gate, high_gate), (train_up, low_up, high_up)),
        lambda share, m, row: (out, share.index((m, row // GROUP)) * GROUP + row % GROUP),
        blocks, lows, highs, load_sems, small_sems, send_sems, recv_sems,
        lambda targets: pl.semaphore_wait(barrier, len(targets)),
        lambda order: None,
    )


def write_first(gate, up, gain, out_gate, out_up, out_gain, sems):
    shares = shares_of(gate.shape[0] // GROUP)
    small = pltpu.make_async_copy(gain, out_gain, sems.at[2])
    small.start()

    def run(share):
        pairs = ((gate, out_gate), (up, out_up))
        ends = [GROUP * sum(m == k for m, _ in share) for k in range(2)]
        for k in range(PARTS):
            for m, (source, target) in enumerate(pairs):
                first, last = (ends[m] // GROUP * n // PARTS * GROUP for n in (k, k + 1))
                if last > first:
                    part = pl.ds(first, last - first)
                    pltpu.make_async_copy(source.at[part], target.at[part], sems.at[m]).start()
        for m, (source, target) in enumerate(pairs):
            part = pl.ds(0, ends[m])
            pltpu.make_async_copy(source.at[part], target.at[part], sems.at[m]).wait()

    for core, (share, _) in enumerate(shares):
        pl.when(lax.axis_index("c") == core)(functools.partial(run, share))
    small.wait()


def write_second(rest, held_gate, held_up, out_gate, out_up, sems):
    shares = shares_of(out_gate.shape[0] // GROUP)

    def run(share):
        copies = []
        for k, (m, g) in enumerate(share):
            source = rest.at[pl.ds(k * GROUP, GROUP)]
            target = (out_gate, out_up)[m].at[pl.ds(g * GROUP, GROUP)]
            copies.append(pltpu.make_async_copy(source, target, sems.at[k]))
            copies[-1].start()
        for copy in copies:
            copy.wait()

    for core, (_, share) in enumerate(shares):
        pl.when(lax.axis_index("c") == core)(functools.partial(run, share))


def per_device(train_gate, low_gate, high_gate, train_up, low_up, high_up, norm_train, norm_step):
    rows, width = train_gate.shape
    whole = rows * 8
    rank = low_gate.shape[1]
    most = max(2 * width // GROUP - count for count in FIRST)
    vmem = pl.BlockSpec(memory_space=pltpu.VMEM)
    hbm = pl.BlockSpec(memory_space=pltpu.HBM)
    matrix = jax.ShapeDtypeStruct((width, whole), jnp.bfloat16)
    gain = jax.ShapeDtypeStruct((32, 128), jnp.bfloat16)
    sources = [
        pltpu.with_memory_space_constraint(x, pltpu.HBM)
        for x in (
            train_gate, low_gate.T, high_gate, train_up, low_up.T, high_up,
            norm_train.reshape(1, 32), norm_step.reshape(1, 32),
        )
    ]
    scratch = [
        pltpu.VMEM((2, rows, width), jnp.bfloat16),
        pltpu.VMEM((2, rank, rows), jnp.bfloat16),
        pltpu.VMEM((2, rank, width), jnp.bfloat16),
        pltpu.SemaphoreType.DMA((2, 2)),
        pltpu.SemaphoreType.DMA((5,)),
        pltpu.SemaphoreType.DMA((3, DEPTH)),
        pltpu.SemaphoreType.DMA((7, 2)),
    ]
    limit = 12 * 1024 * 1024
    gathered = pl.pallas_call(
        first_kernel,
        out_shape=(matrix, matrix, gain),
        in_specs=[hbm] * 8,
        out_specs=(vmem, vmem, vmem),
        scratch_shapes=scratch
        + [
            pltpu.VMEM((2, 1, 32), jnp.float32),
            pltpu.VMEM((128, 1, 128), jnp.float32),
            pltpu.VMEM((32, 128), jnp.float32),
            pltpu.SemaphoreType.DMA((1,)),
            pltpu.SemaphoreType.DMA((9,)),
            pltpu.SemaphoreType.REGULAR,
        ],
        compiler_params=pltpu.CompilerParams(collective_id=0, has_side_effects=True, vmem_limit_bytes=limit),
        cost_estimate=pl.CostEstimate(flops=10**9, bytes_accessed=2 * 10**7, transcendentals=0),
    )(*sources)
    held_gate, held_up, served = pl.pallas_call(
        write_first,
        out_shape=(matrix, matrix, gain),
        in_specs=[vmem] * 3,
        out_specs=(hbm, hbm, hbm),
        scratch_shapes=[pltpu.SemaphoreType.DMA((3,))],
        compiler_params=pltpu.CompilerParams(vmem_limit_bytes=limit),
        cost_estimate=pl.CostEstimate(flops=10**7, bytes_accessed=3 * 10**7, transcendentals=0),
    )(*gathered)
    rest = pl.pallas_call(
        second_kernel,
        out_shape=jax.ShapeDtypeStruct((most * GROUP, whole), jnp.bfloat16),
        in_specs=[hbm] * 7,
        out_specs=vmem,
        scratch_shapes=scratch,
        compiler_params=pltpu.CompilerParams(collective_id=1, has_side_effects=True, vmem_limit_bytes=limit),
        cost_estimate=pl.CostEstimate(flops=10**9, bytes_accessed=2 * 10**7, transcendentals=0),
    )(*sources[:6], pltpu.with_memory_space_constraint(served, pltpu.HBM))
    ready_gate, ready_up = pl.pallas_call(
        write_second,
        out_shape=(matrix, matrix),
        in_specs=[vmem, hbm, hbm],
        out_specs=(hbm, hbm),
        input_output_aliases={1: 0, 2: 1},
        scratch_shapes=[pltpu.SemaphoreType.DMA((most,))],
        compiler_params=pltpu.CompilerParams(vmem_limit_bytes=limit),
        cost_estimate=pl.CostEstimate(flops=10**7, bytes_accessed=10**7, transcendentals=0),
    )(rest, held_gate, held_up)
    return (ready_gate, ready_up, served.reshape(-1))


def solution(mesh):
    finer = Mesh(mesh.devices.reshape(SIZES), AXES)
    placed = (
        P(SHARD, COLS),
        P(SHARD, None),
        P(None, COLS),
        P(SHARD, COLS),
        P(SHARD, None),
        P(None, COLS),
        P(SHARD + COLS),
        P(SHARD + COLS),
    )
    return jax.shard_map(
        per_device,
        mesh=finer,
        in_specs=placed,
        out_specs=(P(COLS, None), P(COLS, None), P()),
        check_vma=False,
    )
```

```python
import functools

import jax
import jax.numpy as jnp
from jax import lax
from jax.experimental import pallas as pl
from jax.experimental.pallas import tpu as pltpu
from jax.sharding import Mesh
from jax.sharding import PartitionSpec as P

MESH = pl.DeviceIdType.MESH
AXES = ("y", "xl", "z", "xh", "c")
SHARD = ("y", "xl")
COLS = ("z", "xh", "c")
SIZES = (4, 2, 4, 2, 2)

mix_rate = 1.0

GROUP = 128
CHUNK = 64
PARTS = 4
DEPTH = 4
FIRST = (9, 12)
GAIN_EVERY = 8

OWN, BACK, AHEAD, FAR = (0, 0), (3, 0), (1, 0), (2, 0)


def shares_of(groups):
    every = [(m, g) for g in range(groups) for m in range(2)]
    return [(every[:count], every[count:]) for count in FIRST]


def chunks_of(share):
    pieces = [(m, g * GROUP + k, CHUNK) for m, g in share for k in range(0, GROUP, CHUNK)]
    kinds = ([], [])
    for k, piece in enumerate(pieces):
        kinds[0 if (k * 5) % 9 < 5 else 1].append(piece)
    excess = sum(piece[2] for piece in kinds[0]) - (len(share) * GROUP * 5 + 72) // 144 * 16
    if excess:
        giver, taker = kinds if excess > 0 else kinds[::-1]
        m, row, rows = giver.pop()
        giver.append((m, row, rows - abs(excess)))
        taker.append((m, row + rows - abs(excess), abs(excess)))
    return kinds


def plan_of(kinds, partners_first):
    first, second = kinds
    up, down, across = [], [], []

    def add(link, held, seen, kind, pieces):
        link.extend((held, seen, kind, piece) for piece in pieces)

    for kind in (1, 0):
        add(up, OWN, BACK, kind, kinds[kind])
        add(down, OWN, AHEAD, kind, kinds[kind])
    for partners in (partners_first, not partners_first):
        if partners:
            add(up, (0, 1), (3, 1), 0, first)
            add(down, (0, 1), (1, 1), 0, first)
        else:
            add(up, BACK, FAR, 1, second[0::2])
            add(down, AHEAD, FAR, 1, second[1::2])
    add(up, BACK, FAR, 0, first[0::2])
    add(down, AHEAD, FAR, 0, first[1::2])
    add(up, (3, 1), (2, 1), 0, first[1::2])
    add(down, (1, 1), (2, 1), 0, first[0::2])
    add(across, OWN, (0, 1), 0, first)
    for held in (OWN, BACK, AHEAD, FAR):
        add(across, held, (held[0], 1), 1, second)
    return up, down, across


def in_turn(links):
    places, loads = [0] * len(links), [0] * len(links)
    while any(place < len(link) for place, link in zip(places, links)):
        k = min((loads[k], k) for k in range(len(links)) if places[k] < len(links[k]))[1]
        item = links[k][places[k]]
        yield (k, *item)
        places[k] += 1
        loads[k] += item[-1][2]


def greet(sem, *peers):
    for p in peers:
        pl.semaphore_signal(sem, inc=1, device_id=p, device_id_type=MESH)


def only(condition, act):
    if condition is None:
        act()
    else:
        pl.when(condition)(act)


def pass_rows(partners_first, shares, sources, window, blocks, lows, highs, load_sems, small_sems, send_sems, recv_sems, enter, between):
    y, xl, c = (lax.axis_index(name) for name in ("y", "xl", "c"))
    rows = sources[0][0].shape[0]
    across_x = 1 - xl
    targets = ({"y": lax.rem(y + 1, 4)}, {"y": lax.rem(y + 3, 4)}, {"xl": across_x})

    def columns_of(owner):
        column = lax.rem(y + owner[0], 4) * 2 + (across_x if owner[1] else xl)
        return pl.ds(pl.multiple_of(column * rows, rows), rows)

    def run(core, share):
        loads = {}

        def load(m, groups, sem, small):
            train, low, high = sources[m]
            span = pl.ds(groups[0] * GROUP, len(groups) * GROUP)
            started = [pltpu.make_async_copy(train.at[:, span], blocks.at[m, :, span], load_sems.at[m, sem])]
            if small:
                started.append(pltpu.make_async_copy(high, highs.at[m], small_sems.at[2 * m]))
                started.append(pltpu.make_async_copy(low, lows.at[m], small_sems.at[2 * m + 1]))
            for copy in started:
                copy.start()
            loads[m, groups[0]] = started

        mine = [[g for m, g in share if m == k] for k in range(2)]
        order = (share[0][0], 1 - share[0][0])
        for m in order:
            if mine[m]:
                load(m, mine[m][:1], 0, True)
        for m in order:
            if mine[m][1:]:
                load(m, mine[m][1:], 1, False)

        def merge(m, g):
            for copy in loads.get((m, g), ()):
                copy.wait()
            span = pl.ds(g * GROUP, GROUP)
            high = highs[m, :, span].astype(jnp.float32).T.astype(jnp.bfloat16)
            product = jnp.dot(high, lows[m], preferred_element_type=jnp.float32)
            latest = blocks[m, :, span].T.astype(jnp.float32) + mix_rate * product
            ref, row = window(share, m, g * GROUP)
            ref[pl.ds(row, GROUP), columns_of(OWN)] = latest.astype(jnp.bfloat16)

        kinds = chunks_of(share)
        totals = [sum(piece[2] for piece in pieces) for pieces in kinds]
        merged, arrived = set(), set()
        sent = ([], [], [])

        def merge_piece(piece):
            at = (piece[0], piece[1] // GROUP)
            if at not in merged:
                merged.add(at)
                merge(*at)

        def receive(owner, kind):
            if (owner, kind) not in arrived:
                arrived.add((owner, kind))
                as_many = window(share, share[0][0], share[0][1] * GROUP)[0].at[pl.ds(0, totals[kind] // 2), pl.ds(0, 2 * rows)]
                sem = recv_sems.at[owner[0] * 2 + owner[1] - 1, kind]
                pltpu.make_async_copy(as_many, as_many, sem).wait()

        def send(link, held, seen, kind, piece):
            order = len(sent[link])
            if order >= DEPTH:
                sent[link][order - DEPTH].wait_send()
            if held == OWN:
                merge_piece(piece)
            else:
                receive(held, kind)
            m, row, count = piece
            ref, row = window(share, m, row)
            part = ref.at[pl.ds(row, count), columns_of(held)]
            copy = pltpu.make_async_remote_copy(
                src_ref=part,
                dst_ref=part,
                send_sem=send_sems.at[link, order % DEPTH],
                recv_sem=recv_sems.at[seen[0] * 2 + seen[1] - 1, kind],
                device_id=targets[link],
                device_id_type=MESH,
            )
            copy.start()
            sent[link].append(copy)

        merge_piece(kinds[1][0])
        merge_piece(kinds[0][0])
        enter(targets)
        for order, item in enumerate(in_turn(plan_of(kinds, partners_first))):
            send(*item)
            between(order)
        for copies in sent:
            for copy in copies[-DEPTH:]:
                copy.wait_send()
        for oy in range(4):
            for ox in range(2):
                if (oy, ox) != OWN:
                    receive((oy, ox), 0)
                    receive((oy, ox), 1)

    for core, share in enumerate(shares):
        pl.when(c == core)(functools.partial(run, core, share))


def first_kernel(
    train_gate, low_gate, high_gate, train_up, low_up, high_up, norm_train, norm_step,
    out_gate, out_up, out_norm,
    blocks, lows, highs, load_sems, small_sems, send_sems, recv_sems,
    norms, gains, packed, gain_sends, gain_recvs, ready,
):
    y, xl, z, xh, c = (lax.axis_index(name) for name in AXES)
    y_next, y_last = lax.rem(y + 1, 4), lax.rem(y + 3, 4)
    across_x = 1 - xl
    targets = ({"y": y_next}, {"y": y_last}, {"xl": across_x})
    neighbours = ((y_next, xl), (y_last, xl), (y, across_x))

    def at_gate(yy, xx):
        return jnp.logical_and(yy == 1, xx == 0)

    hub_group = jnp.logical_and(xh == 1, c == 1)
    gate = at_gate(y, xl)
    hub = jnp.logical_and(gate, hub_group)
    speaker = jnp.logical_and(gate, jnp.logical_not(hub_group))
    nearby = [jnp.logical_and(hub_group, at_gate(*place)) for place in neighbours]
    other_hubs = [{"z": lax.rem(z + k, 4)} for k in (1, 3, 2)]
    speakers = [{"c": 0}, {"xh": 0}, {"xh": 0, "c": 0}]
    barrier = pltpu.get_barrier_semaphore()

    for target, is_hub in zip(targets, nearby):
        pl.when(jnp.logical_not(is_hub))(functools.partial(greet, barrier, target))
    pl.when(hub)(functools.partial(greet, barrier, *other_hubs))
    pl.when(speaker)(functools.partial(greet, barrier, {"xh": 1, "c": 1}))
    for k, norm in enumerate((norm_train, norm_step)):
        pltpu.make_async_copy(norm, norms.at[k], small_sems.at[4]).start()

    def enter(targets):
        @pl.when(hub)
        def _():
            pl.semaphore_wait(ready, len(targets))

        @pl.when(jnp.logical_not(hub))
        def _():
            pl.semaphore_wait(barrier, len(targets))
            for target, is_hub in zip(targets, nearby):
                pl.when(is_hub)(functools.partial(greet, ready, target))

    col = (z * 2 + xh) * 2 + c
    me = col * 8 + y * 2 + xl
    gain_steps = (
        (None, gains.at[pl.ds(me, 1)], targets[2:], None, 1),
        (None, gains.at[pl.ds(me // 2 * 2, 2)], targets[:2], None, 4),
        (None, gains.at[pl.ds(col * 8 + y_last * 2, 2)], targets[:1], None, 2),
        (speaker, gains.at[pl.ds(col * 8, 8)], [{"xh": 1, "c": 1}], hub, 24),
        (hub, gains.at[pl.ds(z * 32, 32)], other_hubs, hub, 96),
        (hub, out_norm, speakers, speaker, 16),
        (gate, out_norm, targets[2:], jnp.logical_and(y == 1, xl == 1), 16),
        (y == 1, out_norm, targets[:2], jnp.logical_or(y == 0, y == 2), 16),
        (y == 2, out_norm, targets[:1], y == 3, 16),
    )

    def settle(sem, count):
        as_many = gains.at[pl.ds(0, count)]
        pltpu.make_async_copy(as_many, as_many, sem).wait()

    def pack():
        lane = lax.broadcasted_iota(jnp.int32, (1, 128), 1) // 32
        for r in range(32):
            first = r % 4 * 32 + r // 4
            row = gains[first]
            for k in range(1, 4):
                row = jnp.where(lane == k, pltpu.roll(gains[first + 8 * k], 32 * k, 1), row)
            packed[r : r + 1, :] = row
        out_norm[...] = packed[...].astype(jnp.bfloat16)

    def meet():
        pl.semaphore_wait(barrier, len(other_hubs) + len(speakers))
        greet(ready, *speakers)

    def pass_gains(step):
        if step == 0:
            pltpu.make_async_copy(norms, norms, small_sems.at[4]).wait()
            gains[me] = jnp.zeros((1, 128), jnp.float32)
            gains[me, :, 0:32] = norms[0] + norms[1]
            only(hub, meet)
            return
        if step > 1:
            senders, part, peers, receivers, received = gain_steps[step - 2]
            count = 16 if part is out_norm else part.shape[0]
            only(senders, functools.partial(settle, gain_sends.at[0], count * len(peers)))
            only(receivers, functools.partial(settle, gain_recvs.at[step - 2], received))
        if step <= len(gain_steps):
            senders, part, peers, _, _ = gain_steps[step - 1]

            def start():
                if step == 4:
                    pl.semaphore_wait(ready, 1)
                if step == 6:
                    pack()
                for p in peers:
                    pltpu.make_async_remote_copy(
                        src_ref=part,
                        dst_ref=part,
                        send_sem=gain_sends.at[0],
                        recv_sem=gain_recvs.at[step - 1],
                        device_id=p,
                        device_id_type=MESH,
                    ).start()

            only(senders, start)

    def between(order):
        step, rest = divmod(order - 24, GAIN_EVERY)
        if step >= 0 and rest == 0 and step <= len(gain_steps) + 1:
            pass_gains(step)

    outs = (out_gate, out_up)
    pass_rows(
        False,
        [first for first, _ in shares_of(train_gate.shape[1] // GROUP)],
        ((train_gate, low_gate, high_gate), (train_up, low_up, high_up)),
        lambda share, m, row: (outs[m], row),
        blocks, lows, highs, load_sems, small_sems, send_sems, recv_sems, enter, between,
    )


def second_kernel(
    train_gate, low_gate, high_gate, train_up, low_up, high_up, after,
    out,
    blocks, lows, highs, load_sems, small_sems, send_sems, recv_sems,
):
    y, xl = lax.axis_index("y"), lax.axis_index("xl")
    barrier = pltpu.get_barrier_semaphore()
    greet(barrier, {"y": lax.rem(y + 1, 4)}, {"y": lax.rem(y + 3, 4)}, {"xl": 1 - xl})
    pass_rows(
        True,
        [second for _, second in shares_of(train_gate.shape[1] // GROUP)],
        ((train_gate, low_gate, high_gate), (train_up, low_up, high_up)),
        lambda share, m, row: (out, share.index((m, row // GROUP)) * GROUP + row % GROUP),
        blocks, lows, highs, load_sems, small_sems, send_sems, recv_sems,
        lambda targets: pl.semaphore_wait(barrier, len(targets)),
        lambda order: None,
    )


def write_first(gate, up, gain, out_gate, out_up, out_gain, sems):
    shares = shares_of(gate.shape[0] // GROUP)
    small = pltpu.make_async_copy(gain, out_gain, sems.at[2])
    small.start()

    def run(share):
        pairs = ((gate, out_gate), (up, out_up))
        ends = [GROUP * sum(m == k for m, _ in share) for k in range(2)]
        for k in range(PARTS):
            for m, (source, target) in enumerate(pairs):
                first, last = (ends[m] // GROUP * n // PARTS * GROUP for n in (k, k + 1))
                if last > first:
                    part = pl.ds(first, last - first)
                    pltpu.make_async_copy(source.at[part], target.at[part], sems.at[m]).start()
        for m, (source, target) in enumerate(pairs):
            part = pl.ds(0, ends[m])
            pltpu.make_async_copy(source.at[part], target.at[part], sems.at[m]).wait()

    for core, (share, _) in enumerate(shares):
        pl.when(lax.axis_index("c") == core)(functools.partial(run, share))
    small.wait()


def write_second(rest, held_gate, held_up, out_gate, out_up, sems):
    shares = shares_of(out_gate.shape[0] // GROUP)

    def run(share):
        half = GROUP // 2
        for k, (m, g) in enumerate(share):
            for part in range(0, GROUP, half):
                source = rest.at[pl.ds(k * GROUP + part, half)]
                target = (out_gate, out_up)[m].at[pl.ds(g * GROUP + part, half)]
                pltpu.make_async_copy(source, target, sems.at[0]).start()
        whole = rest.at[pl.ds(0, len(share) * GROUP)]
        target = out_gate.at[pl.ds(0, len(share) * GROUP)]
        pltpu.make_async_copy(whole, target, sems.at[0]).wait()

    for core, (_, share) in enumerate(shares):
        pl.when(lax.axis_index("c") == core)(functools.partial(run, share))


def per_device(train_gate, low_gate, high_gate, train_up, low_up, high_up, norm_train, norm_step):
    rows, width = train_gate.shape
    whole = rows * 8
    rank = low_gate.shape[1]
    most = max(2 * width // GROUP - count for count in FIRST)
    vmem = pl.BlockSpec(memory_space=pltpu.VMEM)
    hbm = pl.BlockSpec(memory_space=pltpu.HBM)
    matrix = jax.ShapeDtypeStruct((width, whole), jnp.bfloat16)
    gain = jax.ShapeDtypeStruct((32, 128), jnp.bfloat16)
    sources = [
        pltpu.with_memory_space_constraint(x, pltpu.HBM)
        for x in (
            train_gate, low_gate.T, high_gate, train_up, low_up.T, high_up,
            norm_train.reshape(1, 32), norm_step.reshape(1, 32),
        )
    ]
    scratch = [
        pltpu.VMEM((2, rows, width), jnp.bfloat16),
        pltpu.VMEM((2, rank, rows), jnp.bfloat16),
        pltpu.VMEM((2, rank, width), jnp.bfloat16),
        pltpu.SemaphoreType.DMA((2, 2)),
        pltpu.SemaphoreType.DMA((5,)),
        pltpu.SemaphoreType.DMA((3, DEPTH)),
        pltpu.SemaphoreType.DMA((7, 2)),
    ]
    limit = 12 * 1024 * 1024
    gathered = pl.pallas_call(
        first_kernel,
        out_shape=(matrix, matrix, gain),
        in_specs=[hbm] * 8,
        out_specs=(vmem, vmem, vmem),
        scratch_shapes=scratch
        + [
            pltpu.VMEM((2, 1, 32), jnp.float32),
            pltpu.VMEM((128, 1, 128), jnp.float32),
            pltpu.VMEM((32, 128), jnp.float32),
            pltpu.SemaphoreType.DMA((1,)),
            pltpu.SemaphoreType.DMA((9,)),
            pltpu.SemaphoreType.REGULAR,
        ],
        compiler_params=pltpu.CompilerParams(collective_id=0, has_side_effects=True, vmem_limit_bytes=limit),
        cost_estimate=pl.CostEstimate(flops=10**9, bytes_accessed=2 * 10**7, transcendentals=0),
    )(*sources)
    held_gate, held_up, served = pl.pallas_call(
        write_first,
        out_shape=(matrix, matrix, gain),
        in_specs=[vmem] * 3,
        out_specs=(hbm, hbm, hbm),
        scratch_shapes=[pltpu.SemaphoreType.DMA((3,))],
        compiler_params=pltpu.CompilerParams(vmem_limit_bytes=limit),
        cost_estimate=pl.CostEstimate(flops=10**7, bytes_accessed=3 * 10**7, transcendentals=0),
    )(*gathered)
    rest = pl.pallas_call(
        second_kernel,
        out_shape=jax.ShapeDtypeStruct((most * GROUP, whole), jnp.bfloat16),
        in_specs=[hbm] * 7,
        out_specs=vmem,
        scratch_shapes=scratch,
        compiler_params=pltpu.CompilerParams(collective_id=1, has_side_effects=True, vmem_limit_bytes=limit),
        cost_estimate=pl.CostEstimate(flops=10**9, bytes_accessed=2 * 10**7, transcendentals=0),
    )(*sources[:6], pltpu.with_memory_space_constraint(served, pltpu.HBM))
    ready_gate, ready_up = pl.pallas_call(
        write_second,
        out_shape=(matrix, matrix),
        in_specs=[vmem, hbm, hbm],
        out_specs=(hbm, hbm),
        input_output_aliases={1: 0, 2: 1},
        scratch_shapes=[pltpu.SemaphoreType.DMA((1,))],
        compiler_params=pltpu.CompilerParams(vmem_limit_bytes=limit),
        cost_estimate=pl.CostEstimate(flops=10**7, bytes_accessed=10**7, transcendentals=0),
    )(rest, held_gate, held_up)
    return (ready_gate, ready_up, served.reshape(-1))


def solution(mesh):
    finer = Mesh(mesh.devices.reshape(SIZES), AXES)
    placed = (
        P(SHARD, COLS),
        P(SHARD, None),
        P(None, COLS),
        P(SHARD, COLS),
        P(SHARD, None),
        P(None, COLS),
        P(SHARD + COLS),
        P(SHARD + COLS),
    )
    return jax.shard_map(
        per_device,
        mesh=finer,
        in_specs=placed,
        out_specs=(P(COLS, None), P(COLS, None), P()),
        check_vma=False,
    )
```

```python
import functools

import jax
import jax.numpy as jnp
from jax import lax
from jax.experimental import pallas as pl
from jax.experimental.pallas import tpu as pltpu
from jax.sharding import Mesh
from jax.sharding import PartitionSpec as P

MESH = pl.DeviceIdType.MESH
AXES = ("y", "xl", "z", "xh", "c")
SHARD = ("y", "xl")
COLS = ("z", "xh", "c")
SIZES = (4, 2, 4, 2, 2)

mix_rate = 1.0

GROUP = 128
CHUNK = 64
PARTS = 4
DEPTH = 4
FIRST = (9, 12)
GAIN_EVERY = 8

OWN, BACK, AHEAD, FAR = (0, 0), (3, 0), (1, 0), (2, 0)


def shares_of(groups):
    every = [(m, g) for g in range(groups) for m in range(2)]
    return [(every[:count], every[count:]) for count in FIRST]


def chunks_of(share):
    pieces = [(m, g * GROUP + k, CHUNK) for m, g in share for k in range(0, GROUP, CHUNK)]
    kinds = ([], [])
    for k, piece in enumerate(pieces):
        kinds[0 if (k * 5) % 9 < 5 else 1].append(piece)
    excess = sum(piece[2] for piece in kinds[0]) - (len(share) * GROUP * 5 + 72) // 144 * 16
    if excess:
        giver, taker = kinds if excess > 0 else kinds[::-1]
        m, row, rows = giver.pop()
        giver.append((m, row, rows - abs(excess)))
        taker.append((m, row + rows - abs(excess), abs(excess)))
    return kinds


def plan_of(kinds):
    first, second = kinds
    up, down, across = [], [], []

    def add(link, held, seen, kind, pieces):
        link.extend((held, seen, kind, piece) for piece in pieces)

    for kind in (1, 0):
        add(up, OWN, BACK, kind, kinds[kind])
        add(down, OWN, AHEAD, kind, kinds[kind])
    add(up, BACK, FAR, 1, second[0::2])
    add(down, AHEAD, FAR, 1, second[1::2])
    add(up, (0, 1), (3, 1), 0, first)
    add(down, (0, 1), (1, 1), 0, first)
    add(up, BACK, FAR, 0, first[0::2])
    add(down, AHEAD, FAR, 0, first[1::2])
    add(up, (3, 1), (2, 1), 0, first[1::2])
    add(down, (1, 1), (2, 1), 0, first[0::2])
    add(across, OWN, (0, 1), 0, first)
    for held in (OWN, BACK, AHEAD, FAR):
        add(across, held, (held[0], 1), 1, second)
    return up, down, across


def in_turn(links):
    places, loads = [0] * len(links), [0] * len(links)
    while any(place < len(link) for place, link in zip(places, links)):
        k = min((loads[k], k) for k in range(len(links)) if places[k] < len(links[k]))[1]
        item = links[k][places[k]]
        yield (k, *item)
        places[k] += 1
        loads[k] += item[-1][2]


def greet(sem, *peers):
    for p in peers:
        pl.semaphore_signal(sem, inc=1, device_id=p, device_id_type=MESH)


def only(condition, act):
    if condition is None:
        act()
    else:
        pl.when(condition)(act)


def pass_rows(shares, sources, window, blocks, lows, highs, load_sems, small_sems, send_sems, recv_sems, begin, enter, between):
    y, xl, c = (lax.axis_index(name) for name in ("y", "xl", "c"))
    rows = sources[0][0].shape[0]
    across_x = 1 - xl
    targets = ({"y": lax.rem(y + 1, 4)}, {"y": lax.rem(y + 3, 4)}, {"xl": across_x})

    def columns_of(owner):
        column = lax.rem(y + owner[0], 4) * 2 + (across_x if owner[1] else xl)
        return pl.ds(pl.multiple_of(column * rows, rows), rows)

    def run(core, share):
        loads = {}

        def load(m, groups, sem, small):
            train, low, high = sources[m]
            span = pl.ds(groups[0] * GROUP, len(groups) * GROUP)
            started = [pltpu.make_async_copy(train.at[:, span], blocks.at[m, :, span], load_sems.at[m, sem])]
            if small:
                started.append(pltpu.make_async_copy(high, highs.at[m], small_sems.at[2 * m]))
                started.append(pltpu.make_async_copy(low, lows.at[m], small_sems.at[2 * m + 1]))
            for copy in started:
                copy.start()
            loads[m, groups[0]] = started

        mine = [[g for m, g in share if m == k] for k in range(2)]
        order = (share[0][0], 1 - share[0][0])
        for m in order:
            if mine[m]:
                load(m, mine[m][:1], 0, True)
                if m == order[0]:
                    begin()
        for m in order:
            if mine[m][1:]:
                load(m, mine[m][1:], 1, False)

        def merge(m, g):
            for copy in loads.get((m, g), ()):
                copy.wait()
            span = pl.ds(g * GROUP, GROUP)
            high = highs[m, :, span].astype(jnp.float32).T.astype(jnp.bfloat16)
            product = jnp.dot(high, lows[m], preferred_element_type=jnp.float32)
            latest = blocks[m, :, span].T.astype(jnp.float32) + mix_rate * product
            ref, row = window(share, m, g * GROUP)
            ref[pl.ds(row, GROUP), columns_of(OWN)] = latest.astype(jnp.bfloat16)

        kinds = chunks_of(share)
        totals = [sum(piece[2] for piece in pieces) for pieces in kinds]
        merged, arrived = set(), set()
        sent = ([], [], [])

        def merge_piece(piece):
            at = (piece[0], piece[1] // GROUP)
            if at not in merged:
                merged.add(at)
                merge(*at)

        def receive(owner, kind):
            if (owner, kind) not in arrived:
                arrived.add((owner, kind))
                as_many = window(share, share[0][0], share[0][1] * GROUP)[0].at[pl.ds(0, totals[kind] // 2), pl.ds(0, 2 * rows)]
                sem = recv_sems.at[owner[0] * 2 + owner[1] - 1, kind]
                pltpu.make_async_copy(as_many, as_many, sem).wait()

        def send(link, held, seen, kind, piece):
            order = len(sent[link])
            if order >= DEPTH:
                sent[link][order - DEPTH].wait_send()
            if held == OWN:
                merge_piece(piece)
            else:
                receive(held, kind)
            m, row, count = piece
            ref, row = window(share, m, row)
            part = ref.at[pl.ds(row, count), columns_of(held)]
            copy = pltpu.make_async_remote_copy(
                src_ref=part,
                dst_ref=part,
                send_sem=send_sems.at[link, order % DEPTH],
                recv_sem=recv_sems.at[seen[0] * 2 + seen[1] - 1, kind],
                device_id=targets[link],
                device_id_type=MESH,
            )
            copy.start()
            sent[link].append(copy)

        merge_piece(kinds[1][0])
        merge_piece(kinds[0][0])
        enter(targets)
        for order, item in enumerate(in_turn(plan_of(kinds))):
            send(*item)
            between(order)
        for copies in sent:
            for copy in copies[-DEPTH:]:
                copy.wait_send()
        for oy in range(4):
            for ox in range(2):
                if (oy, ox) != OWN:
                    receive((oy, ox), 0)
                    receive((oy, ox), 1)

    for core, share in enumerate(shares):
        pl.when(c == core)(functools.partial(run, core, share))


def first_kernel(
    train_gate, low_gate, high_gate, train_up, low_up, high_up, norm_train, norm_step,
    out_gate, out_up, out_norm,
    blocks, lows, highs, load_sems, small_sems, send_sems, recv_sems,
    norms, gains, packed, gain_sends, gain_recvs, ready,
):
    y, xl, z, xh, c = (lax.axis_index(name) for name in AXES)
    y_next, y_last = lax.rem(y + 1, 4), lax.rem(y + 3, 4)
    across_x = 1 - xl
    targets = ({"y": y_next}, {"y": y_last}, {"xl": across_x})
    neighbours = ((y_next, xl), (y_last, xl), (y, across_x))

    def at_gate(yy, xx):
        return jnp.logical_and(yy == 1, xx == 0)

    hub_group = jnp.logical_and(xh == 1, c == 1)
    gate = at_gate(y, xl)
    hub = jnp.logical_and(gate, hub_group)
    speaker = jnp.logical_and(gate, jnp.logical_not(hub_group))
    nearby = [jnp.logical_and(hub_group, at_gate(*place)) for place in neighbours]
    other_hubs = [{"z": lax.rem(z + k, 4)} for k in (1, 3, 2)]
    speakers = [{"c": 0}, {"xh": 0}, {"xh": 0, "c": 0}]
    barrier = pltpu.get_barrier_semaphore()

    def begin():
        for target, is_hub in zip(targets, nearby):
            pl.when(jnp.logical_not(is_hub))(functools.partial(greet, barrier, target))
        pl.when(hub)(functools.partial(greet, barrier, *other_hubs))
        pl.when(speaker)(functools.partial(greet, barrier, {"xh": 1, "c": 1}))
        for k, norm in enumerate((norm_train, norm_step)):
            pltpu.make_async_copy(norm, norms.at[k], small_sems.at[4]).start()

    def enter(targets):
        @pl.when(hub)
        def _():
            pl.semaphore_wait(ready, len(targets))

        @pl.when(jnp.logical_not(hub))
        def _():
            pl.semaphore_wait(barrier, len(targets))
            for target, is_hub in zip(targets, nearby):
                pl.when(is_hub)(functools.partial(greet, ready, target))

    col = (z * 2 + xh) * 2 + c
    me = col * 8 + y * 2 + xl
    gain_steps = (
        (None, gains.at[pl.ds(me, 1)], targets[2:], None, 1),
        (None, gains.at[pl.ds(me // 2 * 2, 2)], targets[:2], None, 4),
        (None, gains.at[pl.ds(col * 8 + y_last * 2, 2)], targets[:1], None, 2),
        (speaker, gains.at[pl.ds(col * 8, 8)], [{"xh": 1, "c": 1}], hub, 24),
        (hub, gains.at[pl.ds(z * 32, 32)], other_hubs, hub, 96),
        (hub, out_norm, speakers, speaker, 16),
        (gate, out_norm, targets[2:], jnp.logical_and(y == 1, xl == 1), 16),
        (y == 1, out_norm, targets[:2], jnp.logical_or(y == 0, y == 2), 16),
        (y == 2, out_norm, targets[:1], y == 3, 16),
    )

    def settle(sem, count):
        as_many = gains.at[pl.ds(0, count)]
        pltpu.make_async_copy(as_many, as_many, sem).wait()

    def pack():
        lane = lax.broadcasted_iota(jnp.int32, (1, 128), 1) // 32
        for r in range(32):
            first = r % 4 * 32 + r // 4
            row = gains[first]
            for k in range(1, 4):
                row = jnp.where(lane == k, pltpu.roll(gains[first + 8 * k], 32 * k, 1), row)
            packed[r : r + 1, :] = row
        out_norm[...] = packed[...].astype(jnp.bfloat16)

    def meet():
        pl.semaphore_wait(barrier, len(other_hubs) + len(speakers))
        greet(ready, *speakers)

    def pass_gains(step):
        if step == 0:
            pltpu.make_async_copy(norms, norms, small_sems.at[4]).wait()
            gains[me] = jnp.zeros((1, 128), jnp.float32)
            gains[me, :, 0:32] = norms[0] + norms[1]
            only(hub, meet)
            return
        if step > 1:
            senders, part, peers, receivers, received = gain_steps[step - 2]
            count = 16 if part is out_norm else part.shape[0]
            only(senders, functools.partial(settle, gain_sends.at[0], count * len(peers)))
            only(receivers, functools.partial(settle, gain_recvs.at[step - 2], received))
        if step <= len(gain_steps):
            senders, part, peers, _, _ = gain_steps[step - 1]

            def start():
                if step == 4:
                    pl.semaphore_wait(ready, 1)
                if step == 6:
                    pack()
                for p in peers:
                    pltpu.make_async_remote_copy(
                        src_ref=part,
                        dst_ref=part,
                        send_sem=gain_sends.at[0],
                        recv_sem=gain_recvs.at[step - 1],
                        device_id=p,
                        device_id_type=MESH,
                    ).start()

            only(senders, start)

    def between(order):
        step, rest = divmod(order - 24, GAIN_EVERY)
        if step >= 0 and rest == 0 and step <= len(gain_steps) + 1:
            pass_gains(step)

    outs = (out_gate, out_up)
    pass_rows(
        [first for first, _ in shares_of(train_gate.shape[1] // GROUP)],
        ((train_gate, low_gate, high_gate), (train_up, low_up, high_up)),
        lambda share, m, row: (outs[m], row),
        blocks, lows, highs, load_sems, small_sems, send_sems, recv_sems, begin, enter, between,
    )


def second_kernel(
    train_gate, low_gate, high_gate, train_up, low_up, high_up, after,
    out,
    blocks, lows, highs, load_sems, small_sems, send_sems, recv_sems,
):
    y, xl = lax.axis_index("y"), lax.axis_index("xl")
    barrier = pltpu.get_barrier_semaphore()
    pass_rows(
        [second for _, second in shares_of(train_gate.shape[1] // GROUP)],
        ((train_gate, low_gate, high_gate), (train_up, low_up, high_up)),
        lambda share, m, row: (out, share.index((m, row // GROUP)) * GROUP + row % GROUP),
        blocks, lows, highs, load_sems, small_sems, send_sems, recv_sems,
        lambda: greet(barrier, {"y": lax.rem(y + 1, 4)}, {"y": lax.rem(y + 3, 4)}, {"xl": 1 - xl}),
        lambda targets: pl.semaphore_wait(barrier, len(targets)),
        lambda order: None,
    )


def write_first(gate, up, gain, out_gate, out_up, out_gain, sems):
    shares = shares_of(gate.shape[0] // GROUP)
    small = pltpu.make_async_copy(gain, out_gain, sems.at[2])
    small.start()

    def run(share):
        pairs = ((gate, out_gate), (up, out_up))
        ends = [GROUP * sum(m == k for m, _ in share) for k in range(2)]
        for k in range(PARTS):
            for m, (source, target) in enumerate(pairs):
                first, last = (ends[m] // GROUP * n // PARTS * GROUP for n in (k, k + 1))
                if last > first:
                    part = pl.ds(first, last - first)
                    pltpu.make_async_copy(source.at[part], target.at[part], sems.at[m]).start()
        for m, (source, target) in enumerate(pairs):
            part = pl.ds(0, ends[m])
            pltpu.make_async_copy(source.at[part], target.at[part], sems.at[m]).wait()

    for core, (share, _) in enumerate(shares):
        pl.when(lax.axis_index("c") == core)(functools.partial(run, share))
    small.wait()


def write_second(rest, held_gate, held_up, out_gate, out_up, sems):
    shares = shares_of(out_gate.shape[0] // GROUP)

    def run(share):
        copies = []
        for k, (m, g) in enumerate(share):
            source = rest.at[pl.ds(k * GROUP, GROUP)]
            target = (out_gate, out_up)[m].at[pl.ds(g * GROUP, GROUP)]
            copies.append(pltpu.make_async_copy(source, target, sems.at[k]))
            copies[-1].start()
        for copy in copies:
            copy.wait()

    for core, (_, share) in enumerate(shares):
        pl.when(lax.axis_index("c") == core)(functools.partial(run, share))


def per_device(train_gate, low_gate, high_gate, train_up, low_up, high_up, norm_train, norm_step):
    rows, width = train_gate.shape
    whole = rows * 8
    rank = low_gate.shape[1]
    most = max(2 * width // GROUP - count for count in FIRST)
    vmem = pl.BlockSpec(memory_space=pltpu.VMEM)
    hbm = pl.BlockSpec(memory_space=pltpu.HBM)
    matrix = jax.ShapeDtypeStruct((width, whole), jnp.bfloat16)
    gain = jax.ShapeDtypeStruct((32, 128), jnp.bfloat16)
    sources = [
        pltpu.with_memory_space_constraint(x, pltpu.HBM)
        for x in (
            train_gate, low_gate.T, high_gate, train_up, low_up.T, high_up,
            norm_train.reshape(1, 32), norm_step.reshape(1, 32),
        )
    ]
    scratch = [
        pltpu.VMEM((2, rows, width), jnp.bfloat16),
        pltpu.VMEM((2, rank, rows), jnp.bfloat16),
        pltpu.VMEM((2, rank, width), jnp.bfloat16),
        pltpu.SemaphoreType.DMA((2, 2)),
        pltpu.SemaphoreType.DMA((5,)),
        pltpu.SemaphoreType.DMA((3, DEPTH)),
        pltpu.SemaphoreType.DMA((7, 2)),
    ]
    limit = 12 * 1024 * 1024
    gathered = pl.pallas_call(
        first_kernel,
        out_shape=(matrix, matrix, gain),
        in_specs=[hbm] * 8,
        out_specs=(vmem, vmem, vmem),
        scratch_shapes=scratch
        + [
            pltpu.VMEM((2, 1, 32), jnp.float32),
            pltpu.VMEM((128, 1, 128), jnp.float32),
            pltpu.VMEM((32, 128), jnp.float32),
            pltpu.SemaphoreType.DMA((1,)),
            pltpu.SemaphoreType.DMA((9,)),
            pltpu.SemaphoreType.REGULAR,
        ],
        compiler_params=pltpu.CompilerParams(collective_id=0, has_side_effects=True, vmem_limit_bytes=limit),
        cost_estimate=pl.CostEstimate(flops=10**9, bytes_accessed=2 * 10**7, transcendentals=0),
    )(*sources)
    held_gate, held_up, served = pl.pallas_call(
        write_first,
        out_shape=(matrix, matrix, gain),
        in_specs=[vmem] * 3,
        out_specs=(hbm, hbm, hbm),
        scratch_shapes=[pltpu.SemaphoreType.DMA((3,))],
        compiler_params=pltpu.CompilerParams(vmem_limit_bytes=limit),
        cost_estimate=pl.CostEstimate(flops=10**7, bytes_accessed=3 * 10**7, transcendentals=0),
    )(*gathered)
    rest = pl.pallas_call(
        second_kernel,
        out_shape=jax.ShapeDtypeStruct((most * GROUP, whole), jnp.bfloat16),
        in_specs=[hbm] * 7,
        out_specs=vmem,
        scratch_shapes=scratch,
        compiler_params=pltpu.CompilerParams(collective_id=1, has_side_effects=True, vmem_limit_bytes=limit),
        cost_estimate=pl.CostEstimate(flops=10**9, bytes_accessed=2 * 10**7, transcendentals=0),
    )(*sources[:6], pltpu.with_memory_space_constraint(served, pltpu.HBM))
    ready_gate, ready_up = pl.pallas_call(
        write_second,
        out_shape=(matrix, matrix),
        in_specs=[vmem, hbm, hbm],
        out_specs=(hbm, hbm),
        input_output_aliases={1: 0, 2: 1},
        scratch_shapes=[pltpu.SemaphoreType.DMA((most,))],
        compiler_params=pltpu.CompilerParams(vmem_limit_bytes=limit),
        cost_estimate=pl.CostEstimate(flops=10**7, bytes_accessed=10**7, transcendentals=0),
    )(rest, held_gate, held_up)
    return (ready_gate, ready_up, served.reshape(-1))


def solution(mesh):
    finer = Mesh(mesh.devices.reshape(SIZES), AXES)
    placed = (
        P(SHARD, COLS),
        P(SHARD, None),
        P(None, COLS),
        P(SHARD, COLS),
        P(SHARD, None),
        P(None, COLS),
        P(SHARD + COLS),
        P(SHARD + COLS),
    )
    return jax.shard_map(
        per_device,
        mesh=finer,
        in_specs=placed,
        out_specs=(P(COLS, None), P(COLS, None), P()),
        check_vma=False,
    )
```
